256 devices in a mesh: rep: 16 (over y_lo, x, core), blk: 16 (over z, y_hi).
Axes of the slice: x: 4, y: 4 (y_hi: 2, y_lo: 2; y = y_hi * 2 + y_lo), z: 8, core: 2. Of those that a mesh axis runs over, the one named last changes fastest.
Arguments:
- features: bfloat16 [2, 4096, 2048], P(None, 'rep'), may hold values from -0.125 to 0.125
- grad_act: bfloat16 [2, 4096, 24576], P(None, 'rep', 'blk'), may hold values from -2.5 to 2.5
- weights: bfloat16 [2048, 24576], P(None, 'blk'), may hold values from -6 to 6
- owner_slot: int32 [16, 48], P('blk'), may hold values from 0 to 47, each once within a row
- factors: float32 [16, 48, 2, 256, 256], P('blk', 'rep'), may hold values from -100 to 250, as said below
- roots: bfloat16 [16, 48, 2, 256, 256], P('blk', 'rep'), may hold values from -1 to 2, as said below
- helper_list: int32 [2, 16, 4], replicated, may hold values from 0 to 95, as said below
Outputs:
- weights_out: bfloat16 [16, 48, 256, 256], P('blk', 'rep')
- roots_out: bfloat16 [16, 48, 2, 256, 256], P('blk', 'rep')
The draws below stay inside these ranges and needn't reach their ends.
Inputs may be any that keep to these rules, and one draw needn't show every extreme that they name: `owner_slot`: each row is a permutation of the slots of one group; slot s belongs to index s // 3 of rep. `factors`: symmetric positive definite. `roots`: Symmetric. `helper_list`: entry [t, h, j] is a factor id as in the reference program, refreshed in step t by index h of blk. In a step every helper has exactly 4 ids, no id appears twice, and no helper has two ids of one group; a group has at most min(6, 16) of its ids in a step.
All inputs are finite; a program needn't handle non-finite values.
Results may differ from the reference program's by a relative error of at most 0.0085.
Values may be sent and summed in bfloat16 or wider, within the bound.
A program may use at most 128 MiB of HBM per device.

```python
import math
import jax
import jax.numpy as jnp
from jax import lax

BLOCK = 256
OWN = 3
STEPS = 2
NEWTON = 3
SLOTS = 4
GROUPS = 16
NBG = 48
ROWS = 2048
COLS = 24576
TOKENS = 4096
N_REP = 16


def helper_round(key):
    per_owner = 2 * OWN
    top_load = min(per_owner, GROUPS)
    lift = top_load - SLOTS
    half_lift = lift // 2
    subkeys = jax.random.split(key, 3)
    owners = jax.random.permutation(subkeys[0], GROUPS).astype(jnp.int32)
    owner_loads = jnp.full((GROUPS,), SLOTS, jnp.int32)
    owner_loads = owner_loads.at[owners[0]].add(lift).at[owners[1]].add(-lift)
    owner_loads = owner_loads.at[owners[2]].add(half_lift).at[owners[3]].add(-half_lift)
    scores = jax.random.randint(subkeys[1], (GROUPS, per_owner), 0, 1 << 20) * per_owner + jnp.arange(per_owner, dtype=jnp.int32)[None, :]
    local_order = jnp.argsort(scores, axis=1).astype(jnp.int32)
    starts = jnp.cumsum(owner_loads) - owner_loads
    position = jnp.arange(per_owner, dtype=jnp.int32)[None, :]
    is_live = position < owner_loads[:, None]
    ranking = starts[:, None] + position
    helpers = jax.random.permutation(subkeys[2], GROUPS).astype(jnp.int32)
    target = jnp.where(is_live, helpers[ranking % GROUPS], GROUPS)
    slot_index = jnp.where(is_live, ranking // GROUPS, 0)
    factor_ids = jnp.arange(GROUPS, dtype=jnp.int32)[:, None] * per_owner + local_order
    listing = jnp.zeros((GROUPS, SLOTS), jnp.int32)
    return listing.at[target.reshape(-1), slot_index.reshape(-1)].set(factor_ids.reshape(-1), mode='drop')


def draw_helper_list(key, part):
    return jnp.stack([helper_round(jax.random.fold_in(key, 101 + step_index)) for step_index in range(STEPS)])


def draw_factors(key, part):
    subkeys = jax.random.split(jax.random.fold_in(key, 7), 2)
    noise = jax.random.uniform(subkeys[0], (GROUPS, NBG, 2, BLOCK, BLOCK), jnp.float32, -math.sqrt(3.0), math.sqrt(3.0))
    spread = jax.random.uniform(subkeys[1], (GROUPS, NBG, 2, BLOCK), jnp.float32, 0.0, math.log(3.2))
    scales = jnp.exp(spread)
    gram = jnp.einsum('gsnij,gsnkj->gsnik', noise, noise) / BLOCK + 0.5 * jnp.eye(BLOCK, dtype=jnp.float32)
    return gram * scales[..., :, None] * scales[..., None, :]


def draw_roots(key, part):
    subkeys = jax.random.split(jax.random.fold_in(key, 11), 2)
    noise = jax.random.uniform(subkeys[0], (GROUPS, NBG, 2, BLOCK, BLOCK), jnp.float32, -1.0, 1.0)
    diagonal = jnp.exp(jax.random.uniform(subkeys[1], (GROUPS, NBG, 2, BLOCK), jnp.float32, math.log(0.4), math.log(1.2)))
    mirrored = (noise + jnp.swapaxes(noise, -1, -2)) * (0.35 / BLOCK ** 0.5)
    return (mirrored + diagonal[..., None] * jnp.eye(BLOCK, dtype=jnp.float32)).astype(jnp.bfloat16)


def steps_of(rng, shape, pieces, least, largest):
    factor_of, own = 1.0, jax.random.fold_in(rng, 6)
    for dim, blocks in pieces:
        steps = jnp.exp(jax.random.uniform(jax.random.fold_in(own, dim), (blocks,), jnp.float32, least / len(pieces), largest / len(pieces)))
        factor_of = factor_of * jnp.repeat(steps, shape[dim] // blocks).reshape([-1 if axis == dim else 1 for axis in range(len(shape))])
    return factor_of


def bell_draw(key, shape, deviation, bound, shards=(), kind=jnp.bfloat16):
    factor_of = steps_of(key, shape, shards, -0.22, 0.18) if shards else 1.0
    values = jax.random.normal(key, shape, jnp.float32) * deviation * factor_of
    return jnp.minimum(jnp.maximum(values, -bound), bound).astype(kind)


def setup_inputs(seed: int = 0) -> dict:
    key_list = jax.random.split(jax.random.key(seed), 8)
    return {
        "features": bell_draw(key_list[0], (STEPS, TOKENS, ROWS), ROWS ** -0.5, 0.125, ((1, 16),)),
        "grad_act": bell_draw(key_list[1], (STEPS, TOKENS, COLS), (max(1, 3 * TOKENS // ROWS)) ** -0.5, 2.5, ((1, 16), (2, 16))),
        "weights": bell_draw(key_list[2], (ROWS, COLS), 1.0, 6.0, ((1, 16),)),
        "owner_slot": jax.vmap(lambda own: jax.random.permutation(own, NBG))(jax.random.split(key_list[3], GROUPS)).reshape((GROUPS, NBG)).astype(jnp.int32),
        "factors": draw_factors(jax.random.fold_in(key_list[7], 71), 0),
        "roots": draw_roots(jax.random.fold_in(key_list[7], 71), 0),
        "helper_list": draw_helper_list(jax.random.fold_in(key_list[7], 71), 0),
    }


RIDGE = 0.001
NORM_EPS = 1e-06
DECAY = 0.95
STEP_SIZE = 0.5

def rounded(value):
    return lax.optimization_barrier(value.astype(jnp.bfloat16))

def exact_dot(first, second):
    return jnp.einsum('...ij,...jk->...ik', first, second, precision=lax.Precision.HIGHEST)

def inverse_root(matrices):
    identity = jnp.eye(matrices.shape[-1], dtype=jnp.float32)
    ridged = matrices + RIDGE * identity
    norm_scale = jnp.sqrt(lax.optimization_barrier(jnp.sum(ridged * ridged, axis=(-2, -1), keepdims=True)) + NORM_EPS)
    current = ridged / norm_scale
    result = identity
    for newton_turn in range(NEWTON):
        factor = (5.0 * identity - current) / 4.0
        if newton_turn == 0:
            result = factor * norm_scale ** (-0.25)
        else:
            result = exact_dot(result, factor)
        if newton_turn + 1 < NEWTON:
            square = exact_dot(factor, factor)
            current = exact_dot(exact_dot(square, square), current)
    return rounded(result)

def silu_slope(value):
    sigmoid = jax.nn.sigmoid(value)
    return sigmoid * (1.0 + value * (1.0 - sigmoid))

def group_gradient(features_now, act_group, weight_slots, block_ids):
    block_size = weight_slots.shape[-1]
    slot_count = weight_slots.shape[0]
    token_count, row_count = features_now.shape
    row_blocks = row_count // block_size
    col_blocks = slot_count // row_blocks
    width = col_blocks * block_size
    ordered = jnp.zeros_like(weight_slots).at[block_ids].set(weight_slots)
    dense = ordered.reshape(row_blocks, col_blocks, block_size, block_size).transpose(0, 2, 1, 3).reshape(row_count, width)
    gate_value = jnp.dot(features_now, dense, preferred_element_type=jnp.float32)
    dgate = (act_group.astype(jnp.float32) * silu_slope(gate_value)).astype(jnp.bfloat16)
    per_rep = token_count // N_REP
    feature_parts = features_now.reshape(N_REP, per_rep, row_count)
    dgate_parts = dgate.reshape(N_REP, per_rep, width)

    def add_part(total, pair):
        partial_value = rounded(jnp.dot(pair[0].T, pair[1], preferred_element_type=jnp.float32))
        return (total + partial_value.astype(jnp.float32), 0)
    summed = lax.scan(add_part, jnp.zeros((row_count, width), jnp.float32), (feature_parts, dgate_parts))[0]
    blocks = summed.reshape(row_blocks, block_size, col_blocks, block_size).transpose(0, 2, 1, 3).reshape(slot_count, block_size, block_size)
    return blocks[block_ids]

def reference(features, grad_act, weights, owner_slot, factors, roots, helper_list):
    group_count, slot_count = owner_slot.shape
    block_size = factors.shape[-1]
    step_count, token_count, row_count = features.shape
    row_blocks = row_count // block_size
    col_blocks = slot_count // row_blocks
    width = col_blocks * block_size
    owned = slot_count // N_REP
    per_owner = 2 * owned
    slot_ids = jnp.arange(slot_count, dtype=jnp.int32)
    block_at = jax.vmap(lambda placing: jnp.zeros((slot_count,), jnp.int32).at[placing].set(slot_ids))(owner_slot)
    grid = weights.reshape(row_blocks, block_size, group_count, col_blocks, block_size).transpose(2, 0, 3, 1, 4)
    grid = grid.reshape(group_count, slot_count, block_size, block_size)
    weight_slots = jax.vmap(lambda blocks, index: blocks[index])(grid, block_at)
    current_factors = factors
    current_roots = roots
    for step_index in range(step_count):
        acts = grad_act[step_index].reshape(token_count, group_count, width).transpose(1, 0, 2)
        features_now = features[step_index]
        grads = lax.map(lambda items: group_gradient(features_now, items[0], items[1], items[2]), (acts, weight_slots, block_at))
        grads_low = rounded(grads)
        left_side = rounded(jnp.einsum('gsij,gsjk->gsik', current_roots[:, :, 0].astype(jnp.float32), grads_low.astype(jnp.float32)))
        shaped = jnp.einsum('gsij,gsjk->gsik', left_side.astype(jnp.float32), current_roots[:, :, 1].astype(jnp.float32))
        grad_norm = jnp.sqrt(lax.optimization_barrier(jnp.sum(grads * grads, axis=(-2, -1), keepdims=True)) + NORM_EPS)
        shaped_norm = jnp.sqrt(lax.optimization_barrier(jnp.sum(shaped * shaped, axis=(-2, -1), keepdims=True)) + NORM_EPS)
        weight_slots = rounded(weight_slots.astype(jnp.float32) - STEP_SIZE * (grad_norm / shaped_norm) * shaped)
        left_stat = exact_dot(grads, jnp.swapaxes(grads, -1, -2))
        right_stat = exact_dot(jnp.swapaxes(grads, -1, -2), grads)
        current_factors = DECAY * current_factors + (1.0 - DECAY) * jnp.stack([left_stat, right_stat], axis=2)
        names = helper_list[step_index].reshape(-1)
        owner_pick = (names // per_owner)[:, None]
        local_ids = names % per_owner
        slot_pick = jnp.arange(N_REP, dtype=jnp.int32)[None, :] * owned + (local_ids // 2)[:, None]
        side_pick = (local_ids % 2)[:, None]
        picked = current_factors[owner_pick, slot_pick, side_pick]
        fresh = lax.map(inverse_root, picked)
        current_roots = current_roots.at[owner_pick, slot_pick, side_pick].set(fresh)
    return (weight_slots, current_roots)
```

```python
import jax
import jax.numpy as jnp
from jax import lax
from jax.experimental import pallas as pl
from jax.experimental.pallas import tpu as pltpu
from jax.sharding import PartitionSpec as P

NEWTON = 3
RIDGE = 0.001
NORM_EPS = 1e-06
DECAY = 0.95
STEP_SIZE = 0.5

B = 256
H = B // 2
OWN = 3
RB = 8
CB = 6
XN = 4
F32 = jnp.float32
BF16 = jnp.bfloat16
MESH = pl.DeviceIdType.MESH

ORDER = (
    [(2, 1, 1), (2, 1, 2), (2, 0, 1), (2, 0, 2)]
    + [(2, 1, 0), (1, 1, 0), (3, 1, 0), (0, 1, 0)]
    + [(1, 1, 2), (3, 1, 1), (1, 0, 2), (3, 0, 1)]
    + [(1, 1, 1), (3, 1, 2), (1, 0, 1), (3, 0, 2)]
    + [(2, 0, 0), (1, 0, 0), (3, 0, 0), (0, 0, 0)]
    + [(0, 1, 1), (0, 1, 2), (0, 0, 1), (0, 0, 2)]
)
PLACE = {item: q for q, item in enumerate(ORDER)}


def transfer_names():
    names = [("x", 0), ("x", 1)]
    for t in range(2):
        names += [("D", t, j) for j in range(CB)]
        names += [("s1", t, way, dy) for way in range(2) for dy in range(2)]
        names += [("a1", t, dx) for dx in range(4)]
        names += [("in", t, way, dy) for way in range(2) for dy in range(2)]
        names += [("de", t, way, dy) for way in range(2) for dy in range(2)]
        names += [(kind, t, way) for kind in ("fa", "ia", "da") for way in range(2)]
        names += [("b2", t, k) for k in (1, 2)]
    names += [(kind, k) for kind in ("yo", "r", "l") for k in range(OWN)]
    names += [(kind, k) for kind in ("rp", "lp") for k in (1, 2)]
    names += [("ya", place) for place in "LRF"]
    names += ["rh", "lh"]
    names += [(kind, dy) for kind in ("rf", "lf") for dy in range(2)]
    names += [("d",) + item for item in ORDER]
    return {name: n for n, name in enumerate(names)}


NAMES = transfer_names()


def dot(first, second):
    return jnp.dot(first, second, preferred_element_type=F32)


def low(value):
    return value.astype(BF16)


def total(value):
    return jnp.sum(value, axis=(0, 1), keepdims=True)


def kernel(
    place, owner, listing, feat, act, wts, fac, rts,
    wout, rout,
    xraw, xpeer, xt0, xt1, wbuf, actb, db0, db1, pb, wg, wown, gbuf, fbuf, qbuf,
    fwdb, froml, fromr, ya, fwda, fromla, fromra, yb,
    ssem, rsem, lsem,
):
    xt, db = (xt0, xt1), (db0, db1)
    r = lax.axis_index("rep")
    group = lax.axis_index("blk")
    c = lax.rem(r, 2)
    x = lax.rem(r // 2, XN)
    y = r // (2 * XN)

    def rep_of(yy, xx, cc):
        return (yy * XN + xx) * 2 + cc

    def right_by(dx):
        return lax.rem(x + dx, XN)

    def y_of(dy):
        return y if dy == 0 else 1 - y

    def slot(dx, dy, cc, k):
        return OWN * rep_of(y_of(dy), right_by(dx), cc) + k

    sib = rep_of(y, x, 1 - c)
    yp = rep_of(1 - y, x, c)
    xr = rep_of(y, right_by(1), c)
    xl = rep_of(y, right_by(3), c)

    def load(n, src, dst):
        copy = pltpu.make_async_copy(src, dst, lsem.at[n])
        copy.start()
        return copy

    def wait_weights(j):
        columns = wbuf.at[pl.ds(j * RB, RB)]
        pltpu.make_async_copy(columns, columns, lsem.at[j]).wait()

    load_x = [load(CB, feat.at[0], xraw.at[0])]
    for j in range(CB):
        for i in range(RB):
            load(j, wts.at[pl.ds(i * B, B), pl.ds(j * B, B)], wbuf.at[j * RB + i])
    load_a = load(CB + 1, act, actb)
    load_x.append(load(CB + 2, feat.at[1], xraw.at[1]))
    load_f = load(CB + 3, fac.at[0], fbuf)
    load_q = load(CB + 4, rts.at[0], qbuf)

    barrier = pltpu.get_barrier_semaphore()
    for partner in (sib, yp, xr, xl):
        pl.semaphore_signal(barrier, inc=1, device_id={"rep": partner}, device_id_type=MESH)
    pl.semaphore_wait(barrier, 4)

    started = []

    def remote(n, src, dst, dev):
        return pltpu.make_async_remote_copy(
            src_ref=src, dst_ref=dst, send_sem=ssem.at[n], recv_sem=rsem.at[n],
            device_id={"rep": dev}, device_id_type=MESH,
        )

    def send(name, src, dst, dev):
        copy = remote(NAMES[name], src, dst, dev)
        copy.start()
        started.append(copy)

    def arrived(name, ref, dev):
        remote(NAMES[name], ref, ref, dev).wait_recv()

    for t in range(2):
        send(("x", t), feat.at[t], xpeer.at[t], sib)

    def transpose(src, t, half):
        def turn(i, carry):
            cols = pl.ds(pl.multiple_of(i * B, B), B)
            xt[t][i, :, half * B:(half + 1) * B] = src[t, :, cols].T
            return carry
        lax.fori_loop(0, RB, turn, 0)

    def gate(t, ready):
        def one(j, carry):
            if ready is not None:
                ready(j)
            value = dot(xraw[t], wbuf[pl.ds(j * RB, RB)].reshape(RB * B, B))
            sigmoid = 1.0 / (1.0 + jnp.exp(-value))
            slope = sigmoid * (1.0 + value * (1.0 - sigmoid))
            cols = pl.ds(pl.multiple_of(j * B, B), B)
            db[t][j, 0:B, :] = low(actb[t, :, cols].astype(F32) * slope)
            remote(
                NAMES[("D", t, 0)] + j, db[t].at[j, pl.ds(0, B), :], db[t].at[j, pl.ds(B, B), :], sib
            ).start()
            return carry
        lax.fori_loop(0, CB, one, 0)
        for j in range(CB):
            own = db[t].at[j, pl.ds(0, B), :]
            other = db[t].at[j, pl.ds(B, B), :]
            started.append(remote(NAMES[("D", t, j)], own, other, sib))
            arrived(("D", t, j), other, sib)

    def partials(t, first, count):
        slots = [slot(dx, dy, c, k) for dx, dy, k in ORDER[first:first + count]]

        def one(n, carry):
            here = slots[0]
            for m in range(1, count):
                here = jnp.where(n == m, slots[m], here)
            pb[t, first + n] = low(dot(xt[t][place[0, here]], db[t][place[1, here]]))
            return carry
        lax.fori_loop(0, count, one, 0)

    def p(t, dx, dy, k):
        return pb.at[t, PLACE[(dx, dy, k)]]

    def reduce_blocks(t, between):
        side = ((xr, 1, xl), (xl, 3, xr))
        partials(t, 0, 4)
        for dy in (1, 0):
            for way in range(2):
                send(("s1", t, way, dy), p(t, 2, dy, 1 + way), fwdb.at[t, way, dy], side[way][0])
        partials(t, 4, 4)
        for dx in (2, 1, 3, 0):
            send(("a1", t, dx), p(t, dx, 1, 0), ya.at[t, dx], yp)
        partials(t, 8, 4)
        land = (froml, fromr)
        for dy in (1, 0):
            for way in range(2):
                k = 2 - way
                send(("in", t, way, dy), p(t, side[way][1], dy, k), land[way].at[t, dy, k - 1], side[way][0])
        for first in (12, 16, 20):
            partials(t, first, 4)
        between()

        def pass_on(dy):
            for way in range(2):
                k = 1 + way
                arrived(("s1", t, way, dy), fwdb.at[t, way, dy], side[way][2])
                mine = p(t, side[way][1], dy, k)
                mine[...] = low(mine[...].astype(F32) + fwdb[t, way, dy].astype(F32))
                send(("de", t, way, dy), mine, land[way].at[t, dy, k - 1], side[way][0])

        def add_y(dx):
            arrived(("a1", t, dx), ya.at[t, dx], yp)
            return p(t, dx, 0, 0)[...].astype(F32) + ya[t, dx].astype(F32)

        halves = (pl.ds(0, H), pl.ds(H, H))
        land_a = (fromla, fromra)
        pass_on(1)
        p(t, 2, 0, 0)[...] = low(add_y(2))
        for way in range(2):
            send(("fa", t, way), p(t, 2, 0, 0).at[halves[way]], fwda.at[t, way], side[way][0])
        pass_on(0)
        for way in range(2):
            dx = side[way][1]
            p(t, dx, 0, 0)[...] = low(add_y(dx))
            send(("ia", t, way), p(t, dx, 0, 0).at[halves[1 - way]], land_a[way].at[t, 1 - way], side[way][0])
        gbuf[0] = add_y(0)
        for way in range(2):
            arrived(("fa", t, way), fwda.at[t, way], side[way][2])
            mine = p(t, side[way][1], 0, 0).at[halves[way]]
            mine[...] = low(mine[...].astype(F32) + fwda[t, way].astype(F32))
            send(("da", t, way), mine, land_a[way].at[t, way], side[way][0])

        def summed(dy, k):
            for way in range(2):
                kind = "de" if k == 1 + way else "in"
                arrived((kind, t, way, dy), land[way].at[t, dy, k - 1], side[way][2])
            return (
                p(t, 0, dy, k)[...].astype(F32)
                + froml[t, dy, k - 1].astype(F32) + fromr[t, dy, k - 1].astype(F32)
            )

        for k in (1, 2):
            p(t, 0, 1, k)[...] = low(summed(1, k))
            send(("b2", t, k), p(t, 0, 1, k), yb.at[t, k - 1], yp)
        for k in (1, 2):
            gbuf[k] = summed(0, k)
        for way in range(2):
            arrived(("ia", t, way), land_a[way].at[t, 1 - way], side[way][2])
            arrived(("da", t, way), land_a[way].at[t, way], side[way][2])
        for half in range(2):
            rows = slice(half * H, (half + 1) * H)
            gbuf[0, rows, :] += fromla[t, half].astype(F32) + fromra[t, half].astype(F32)

    def finish_sum(t, k):
        if k > 0:
            arrived(("b2", t, k), yb.at[t, k - 1], yp)
            gbuf[k] = gbuf[k] + yb[t, k - 1].astype(F32)

    def update(k):
        grad = gbuf[k]
        left = low(dot(qbuf[k, 0], low(grad)))
        shaped = dot(left, qbuf[k, 1])
        grad_norm = jnp.sqrt(total(grad * grad) + NORM_EPS)
        shaped_norm = jnp.sqrt(total(shaped * shaped) + NORM_EPS)
        value = low(wown[k].astype(F32) - STEP_SIZE * (grad_norm / shaped_norm) * shaped)
        wown[k] = value
        return value

    def refresh(t, k):
        grad = low(gbuf[k])
        turned = grad.T
        rows = lax.broadcasted_iota(jnp.int32, (B, B), 0)
        cols = lax.broadcasted_iota(jnp.int32, (B, B), 1)
        diagonal = rows == cols
        five = jnp.where(diagonal, F32(5.0), F32(0.0))
        stats = (dot(grad, turned), dot(turned, grad))
        for e in range(2):
            fresh = DECAY * fbuf[k, e] + (1.0 - DECAY) * stats[e]
            fbuf[k, e] = fresh
            ridged = fresh + jnp.where(diagonal, F32(RIDGE), F32(0.0))
            scale = jnp.sqrt(total(ridged * ridged) + NORM_EPS)
            current = ridged / scale
            factor = (five - current) * 0.25
            result = factor / jnp.sqrt(jnp.sqrt(scale))
            for turn in range(1, NEWTON):
                factor_low = low(factor)
                square = low(dot(factor_low, factor_low))
                current = dot(low(dot(square, square)), low(current))
                factor = (five - current) * 0.25
                result = dot(low(result), low(factor))
            name = group * (2 * OWN) + 2 * k + e
            hits = total(jnp.where(listing[t] == name, F32(1.0), F32(0.0)))
            qbuf[k, e] = jnp.where(hits > 0.5, low(result), qbuf[k, e])

    def w_at(dx, dy, k):
        return wg.at[slot(dx, dy, c, k)]

    def share(dx, dy, k):
        ref = w_at(dx, dy, k)
        send(("d", dx, dy, k), ref, ref, sib)

    def gather_blocks():
        def ship(name, ref, dev):
            send(name, ref, ref, dev)

        for k in range(OWN):
            finish_sum(0, k)
            wg[slot(0, 0, c, k)] = update(k)
            ship(("r", k), w_at(0, 0, k), xr)
            ship(("l", k), w_at(0, 0, k), xl)
            if k > 0:
                ship(("yo", k), w_at(0, 0, k), yp)
            share(0, 0, k)
        ship(("yo", 0), w_at(0, 0, 0), yp)
        refresh(0, 0)
        top, bottom = pl.ds(0, H), pl.ds(H, H)
        arrived(("r", 0), w_at(3, 0, 0), xl)
        ship("rh", w_at(3, 0, 0).at[top], xr)
        ship(("ya", "L"), w_at(3, 0, 0), yp)
        share(3, 0, 0)
        arrived(("l", 0), w_at(1, 0, 0), xr)
        ship("lh", w_at(1, 0, 0).at[bottom], xl)
        ship(("ya", "R"), w_at(1, 0, 0), yp)
        share(1, 0, 0)
        for k in (1, 2):
            arrived(("yo", k), w_at(0, 1, k), yp)
            ship(("rp", k), w_at(0, 1, k), xr)
            ship(("lp", k), w_at(0, 1, k), xl)
            share(0, 1, k)
        refresh(0, 1)
        for k in (1, 2):
            arrived(("r", k), w_at(3, 0, k), xl)
            if k == 1:
                ship(("rf", 0), w_at(3, 0, 1), xr)
            share(3, 0, k)
            arrived(("l", k), w_at(1, 0, k), xr)
            if k == 2:
                ship(("lf", 0), w_at(1, 0, 2), xl)
            share(1, 0, k)
        refresh(0, 2)
        arrived("rh", w_at(2, 0, 0).at[top], xl)
        arrived("lh", w_at(2, 0, 0).at[bottom], xr)
        ship(("ya", "F"), w_at(2, 0, 0), yp)
        share(2, 0, 0)
        arrived(("yo", 0), w_at(0, 1, 0), yp)
        share(0, 1, 0)
        for k in (1, 2):
            arrived(("rp", k), w_at(3, 1, k), xl)
            if k == 1:
                ship(("rf", 1), w_at(3, 1, 1), xr)
            share(3, 1, k)
            arrived(("lp", k), w_at(1, 1, k), xr)
            if k == 2:
                ship(("lf", 1), w_at(1, 1, 2), xl)
            share(1, 1, k)
        arrived(("ya", "L"), w_at(3, 1, 0), yp)
        share(3, 1, 0)
        arrived(("ya", "R"), w_at(1, 1, 0), yp)
        share(1, 1, 0)
        for dy in range(2):
            arrived(("rf", dy), w_at(2, dy, 1), xl)
            share(2, dy, 1)
            arrived(("lf", dy), w_at(2, dy, 2), xr)
            share(2, dy, 2)
        arrived(("ya", "F"), w_at(2, 1, 0), yp)
        share(2, 1, 0)
        for dx, dy, k in ORDER:
            arrived(("d", dx, dy, k), wg.at[slot(dx, dy, 1 - c, k)], sib)

    load_x[0].wait()
    transpose(xraw, 0, 0)
    arrived(("x", 0), xpeer.at[0], sib)
    transpose(xpeer, 0, 1)
    load_a.wait()
    gate(0, wait_weights)
    for k in range(OWN):
        wown[k] = wbuf[place[2, OWN * r + k]]

    def meanwhile():
        load_x[1].wait()
        transpose(xraw, 1, 0)
        arrived(("x", 1), xpeer.at[1], sib)
        transpose(xpeer, 1, 1)

    reduce_blocks(0, meanwhile)
    load_f.wait()
    load_q.wait()
    gather_blocks()

    def lay_out(j, carry):
        for i in range(RB):
            wbuf[j * RB + i] = wg[owner[0, i * CB + j]]
        return carry
    lax.fori_loop(0, CB, lay_out, 0)
    gate(1, None)
    reduce_blocks(1, lambda: None)
    for k in range(OWN):
        finish_sum(1, k)
        wout[0, k] = update(k)
    for k in range(OWN):
        refresh(1, k)
        for e in range(2):
            rout[0, k, e] = qbuf[k, e]
    for copy in started:
        copy.wait_send()


def body(features, grad_act, weights, owner_slot, factors, roots, helper_list):
    ids = jnp.arange(RB * CB, dtype=jnp.int32)
    rows, cols = ids // CB, ids % CB
    kinds = jnp.arange(3, dtype=jnp.int32)[:, None]
    wanted = jnp.where(kinds == 0, rows, jnp.where(kinds == 1, cols, cols * RB + rows))
    placing = owner_slot[0][None, :] == ids[:, None]
    place = jnp.sum(jnp.where(placing[None], wanted[:, None, :], 0), axis=2)
    listing = jnp.swapaxes(helper_list, 1, 2)
    tokens = features.shape[1]
    anywhere = pl.BlockSpec(memory_space=pl.ANY)
    scalars = pl.BlockSpec(memory_space=pltpu.SMEM)
    local = pl.BlockSpec(memory_space=pltpu.VMEM)
    block = (B, B)
    return pl.pallas_call(
        kernel,
        out_shape=(
            jax.ShapeDtypeStruct((1, OWN) + block, BF16),
            jax.ShapeDtypeStruct((1, OWN, 2) + block, BF16),
        ),
        in_specs=[scalars, scalars, local] + [anywhere] * 5,
        out_specs=(local, local),
        scratch_shapes=[
            pltpu.VMEM((2, tokens, RB * B), BF16),
            pltpu.VMEM((2, tokens, RB * B), BF16),
            pltpu.VMEM((RB, B, 2 * tokens), BF16),
            pltpu.VMEM((RB, B, 2 * tokens), BF16),
            pltpu.VMEM((CB * RB,) + block, BF16),
            pltpu.VMEM((2, tokens, CB * B), BF16),
            pltpu.VMEM((CB, 2 * tokens, B), BF16),
            pltpu.VMEM((CB, 2 * tokens, B), BF16),
            pltpu.VMEM((2, len(ORDER)) + block, BF16),
            pltpu.VMEM((RB * CB,) + block, BF16),
            pltpu.VMEM((OWN,) + block, BF16),
            pltpu.VMEM((OWN,) + block, F32),
            pltpu.VMEM((OWN, 2) + block, F32),
            pltpu.VMEM((OWN, 2) + block, BF16),
            pltpu.VMEM((2, 2, 2) + block, BF16),
            pltpu.VMEM((2, 2, 2) + block, BF16),
            pltpu.VMEM((2, 2, 2) + block, BF16),
            pltpu.VMEM((2, 4) + block, BF16),
            pltpu.VMEM((2, 2, H, B), BF16),
            pltpu.VMEM((2, 2, H, B), BF16),
            pltpu.VMEM((2, 2, H, B), BF16),
            pltpu.VMEM((2, 2) + block, BF16),
            pltpu.SemaphoreType.DMA((len(NAMES),)),
            pltpu.SemaphoreType.DMA((len(NAMES),)),
            pltpu.SemaphoreType.DMA((16,)),
        ],
        compiler_params=pltpu.CompilerParams(
            collective_id=0, has_side_effects=True, vmem_limit_bytes=60 * 1024 * 1024
        ),
    )(place, owner_slot, listing, features, grad_act, weights, factors, roots)


def solution(mesh):
    return jax.shard_map(
        body,
        mesh=mesh,
        in_specs=(
            P(None, "rep", None),
            P(None, "rep", "blk"),
            P(None, "blk"),
            P("blk", None),
            P("blk", "rep", None, None, None),
            P("blk", "rep", None, None, None),
            P(),
        ),
        out_specs=(P("blk", "rep", None, None), P("blk", "rep", None, None, None)),
        check_vma=False,
    )
```

```python
import jax
import jax.numpy as jnp
from jax import lax
from jax.experimental import pallas as pl
from jax.experimental.pallas import tpu as pltpu
from jax.sharding import PartitionSpec as P

NEWTON = 3
RIDGE = 0.001
NORM_EPS = 1e-06
DECAY = 0.95
STEP_SIZE = 0.5

B = 256
H = B // 2
OWN = 3
RB = 8
CB = 6
XN = 4
F32 = jnp.float32
BF16 = jnp.bfloat16
MESH = pl.DeviceIdType.MESH

ORDER = (
    [(2, 1, 1), (2, 1, 2), (2, 1, 0), (2, 0, 1), (2, 0, 2)]
    + [(1, 1, 0), (3, 1, 0), (0, 1, 0)]
    + [(1, 1, 2), (3, 1, 1), (1, 1, 1), (3, 1, 2)]
    + [(1, 0, 2), (3, 0, 1), (1, 0, 1), (3, 0, 2)]
    + [(2, 0, 0), (1, 0, 0), (3, 0, 0), (0, 0, 0)]
    + [(0, 1, 1), (0, 1, 2), (0, 0, 1), (0, 0, 2)]
)
PLACE = {item: q for q, item in enumerate(ORDER)}


def transfer_names():
    names = [("x", 0), ("x", 1)]
    for t in range(2):
        names += [("D", t, j) for j in range(CB)]
        names += [("s1", t, way, dy) for way in range(2) for dy in range(2)]
        names += [("a1", t, dx) for dx in range(4)]
        names += [("in", t, way, dy) for way in range(2) for dy in range(2)]
        names += [("de", t, way, dy) for way in range(2) for dy in range(2)]
        names += [(kind, t, way) for kind in ("fa", "ia", "da") for way in range(2)]
        names += [("b2", t, k) for k in (1, 2)]
    names += [(kind, k) for kind in ("yo", "r", "l") for k in range(OWN)]
    names += [(kind, k) for kind in ("rp", "lp") for k in (1, 2)]
    names += [("ya", place) for place in "LRF"]
    names += ["rh", "lh"]
    names += [(kind, dy) for kind in ("rf", "lf") for dy in range(2)]
    names += [("d",) + item for item in ORDER]
    return {name: n for n, name in enumerate(names)}


NAMES = transfer_names()


def dot(first, second):
    return jnp.dot(first, second, preferred_element_type=F32)


def low(value):
    return value.astype(BF16)


def total(value):
    return jnp.sum(value, axis=(0, 1), keepdims=True)


def kernel(
    place, owner, listing, feat, act, wts, fac, rts,
    wout, rout,
    xraw, xpeer, xt0, xt1, wbuf, actb, db0, db1, pb, wg, wown, gbuf, fbuf, qbuf,
    fwdb, froml, fromr, ya, fwda, fromla, fromra, yb,
    ssem, rsem, lsem,
):
    xt, db = (xt0, xt1), (db0, db1)
    r = lax.axis_index("rep")
    group = lax.axis_index("blk")
    c = lax.rem(r, 2)
    x = lax.rem(r // 2, XN)
    y = r // (2 * XN)

    def rep_of(yy, xx, cc):
        return (yy * XN + xx) * 2 + cc

    def right_by(dx):
        return lax.rem(x + dx, XN)

    def y_of(dy):
        return y if dy == 0 else 1 - y

    def slot(dx, dy, cc, k):
        return OWN * rep_of(y_of(dy), right_by(dx), cc) + k

    sib = rep_of(y, x, 1 - c)
    yp = rep_of(1 - y, x, c)
    xr = rep_of(y, right_by(1), c)
    xl = rep_of(y, right_by(3), c)

    def load(n, src, dst):
        copy = pltpu.make_async_copy(src, dst, lsem.at[n])
        copy.start()
        return copy

    def wait_weights(j):
        columns = wbuf.at[pl.ds(j * RB, RB)]
        pltpu.make_async_copy(columns, columns, lsem.at[j]).wait()

    load_x = [load(CB, feat.at[0], xraw.at[0])]
    for j in range(CB):
        for i in range(RB):
            load(j, wts.at[pl.ds(i * B, B), pl.ds(j * B, B)], wbuf.at[j * RB + i])
    load_a = load(CB + 1, act, actb)
    load_x.append(load(CB + 2, feat.at[1], xraw.at[1]))
    load_f = load(CB + 3, fac.at[0], fbuf)
    load_q = load(CB + 4, rts.at[0], qbuf)

    barrier = pltpu.get_barrier_semaphore()
    for partner in (sib, yp, xr, xl):
        pl.semaphore_signal(barrier, inc=1, device_id={"rep": partner}, device_id_type=MESH)
    pl.semaphore_wait(barrier, 4)

    started = []

    def remote(n, src, dst, dev):
        return pltpu.make_async_remote_copy(
            src_ref=src, dst_ref=dst, send_sem=ssem.at[n], recv_sem=rsem.at[n],
            device_id={"rep": dev}, device_id_type=MESH,
        )

    def send(name, src, dst, dev):
        copy = remote(NAMES[name], src, dst, dev)
        copy.start()
        started.append(copy)

    def arrived(name, ref, dev):
        remote(NAMES[name], ref, ref, dev).wait_recv()

    for t in range(2):
        send(("x", t), feat.at[t], xpeer.at[t], sib)

    def transpose(src, t, half):
        def turn(i, carry):
            cols = pl.ds(pl.multiple_of(i * B, B), B)
            xt[t][i, :, half * B:(half + 1) * B] = src[t, :, cols].T
            return carry
        lax.fori_loop(0, RB, turn, 0)

    def gate(t, ready, block):
        def one(j, carry):
            ready(j)
            value = dot(xraw[t, :, 0:B], block(0, j))
            for i in range(1, RB):
                value = value + dot(xraw[t, :, i * B:(i + 1) * B], block(i, j))
            sigmoid = 1.0 / (1.0 + jnp.exp(-value))
            slope = sigmoid * (1.0 + value * (1.0 - sigmoid))
            cols = pl.ds(pl.multiple_of(j * B, B), B)
            db[t][j, 0:B, :] = low(actb[t, :, cols].astype(F32) * slope)
            remote(
                NAMES[("D", t, 0)] + j, db[t].at[j, pl.ds(0, B), :], db[t].at[j, pl.ds(B, B), :], sib
            ).start()
            return carry
        lax.fori_loop(0, CB, one, 0)

    def wait_dgate(t):
        for j in range(CB):
            own = db[t].at[j, pl.ds(0, B), :]
            other = db[t].at[j, pl.ds(B, B), :]
            started.append(remote(NAMES[("D", t, j)], own, other, sib))
            arrived(("D", t, j), other, sib)

    def partial(t, at, here):
        pb[t, at] = low(dot(xt[t][place[0, here]], db[t][place[1, here]]))

    def partials(t, first, count, looped=False):
        slots = [slot(dx, dy, c, k) for dx, dy, k in ORDER[first:first + count]]
        if not looped:
            for m in range(count):
                partial(t, first + m, slots[m])
            return

        def one(n, carry):
            here = slots[0]
            for m in range(1, count):
                here = jnp.where(n == m, slots[m], here)
            partial(t, first + n, here)
            return carry
        lax.fori_loop(0, count, one, 0)

    def p(t, dx, dy, k):
        return pb.at[t, PLACE[(dx, dy, k)]]

    side = ((xr, 1, xl), (xl, 3, xr))
    land = (froml, fromr)
    halves = (pl.ds(0, H), pl.ds(H, H))
    land_a = (fromla, fromra)

    def reduce_blocks(t, between):
        def start(dy):
            for way in range(2):
                send(("s1", t, way, dy), p(t, 2, dy, 1 + way), fwdb.at[t, way, dy], side[way][0])

        def near(dy):
            for way in range(2):
                k = 2 - way
                send(("in", t, way, dy), p(t, side[way][1], dy, k), land[way].at[t, dy, k - 1], side[way][0])

        def across(dx):
            send(("a1", t, dx), p(t, dx, 1, 0), ya.at[t, dx], yp)

        def pass_on(dy):
            for way in range(2):
                k = 1 + way
                arrived(("s1", t, way, dy), fwdb.at[t, way, dy], side[way][2])
                mine = p(t, side[way][1], dy, k)
                mine[...] = low(mine[...].astype(F32) + fwdb[t, way, dy].astype(F32))
                send(("de", t, way, dy), mine, land[way].at[t, dy, k - 1], side[way][0])

        def add_y(dx):
            arrived(("a1", t, dx), ya.at[t, dx], yp)
            return p(t, dx, 0, 0)[...].astype(F32) + ya[t, dx].astype(F32)

        partials(t, 0, 2)
        start(1)
        partials(t, 2, 1)
        across(2)
        partials(t, 3, 2)
        start(0)
        partials(t, 5, 3)
        for dx in (1, 3, 0):
            across(dx)
        partials(t, 8, 4)
        near(1)
        for first in (12, 16, 20):
            partials(t, first, 4, looped=True)
        between()
        pass_on(1)
        p(t, 2, 0, 0)[...] = low(add_y(2))
        for way in range(2):
            send(("fa", t, way), p(t, 2, 0, 0).at[halves[way]], fwda.at[t, way], side[way][0])
        near(0)
        pass_on(0)
        for way in range(2):
            dx = side[way][1]
            p(t, dx, 0, 0)[...] = low(add_y(dx))
            send(("ia", t, way), p(t, dx, 0, 0).at[halves[1 - way]], land_a[way].at[t, 1 - way], side[way][0])
        gbuf[0] = add_y(0)
        for k in (1, 2):
            p(t, 0, 1, k)[...] = low(summed(t, 1, k))
            send(("b2", t, k), p(t, 0, 1, k), yb.at[t, k - 1], yp)
        for way in range(2):
            arrived(("fa", t, way), fwda.at[t, way], side[way][2])
            mine = p(t, side[way][1], 0, 0).at[halves[way]]
            mine[...] = low(mine[...].astype(F32) + fwda[t, way].astype(F32))
            send(("da", t, way), mine, land_a[way].at[t, way], side[way][0])

    def summed(t, dy, k):
        for way in range(2):
            kind = "de" if k == 1 + way else "in"
            arrived((kind, t, way, dy), land[way].at[t, dy, k - 1], side[way][2])
        return (
            p(t, 0, dy, k)[...].astype(F32)
            + froml[t, dy, k - 1].astype(F32) + fromr[t, dy, k - 1].astype(F32)
        )

    def finish_sum(t, k):
        if k > 0:
            value = summed(t, 0, k)
            arrived(("b2", t, k), yb.at[t, k - 1], yp)
            gbuf[k] = value + yb[t, k - 1].astype(F32)
            return
        for way in range(2):
            arrived(("ia", t, way), land_a[way].at[t, 1 - way], side[way][2])
            arrived(("da", t, way), land_a[way].at[t, way], side[way][2])
        for half in range(2):
            rows = slice(half * H, (half + 1) * H)
            gbuf[0, rows, :] += fromla[t, half].astype(F32) + fromra[t, half].astype(F32)

    def update(k):
        grad = gbuf[k]
        left = low(dot(qbuf[k, 0], low(grad)))
        shaped = dot(left, qbuf[k, 1])
        grad_norm = jnp.sqrt(total(grad * grad) + NORM_EPS)
        shaped_norm = jnp.sqrt(total(shaped * shaped) + NORM_EPS)
        value = low(wown[k].astype(F32) - STEP_SIZE * (grad_norm / shaped_norm) * shaped)
        wown[k] = value
        return value

    def refresh(t, owned):
        rows = lax.broadcasted_iota(jnp.int32, (B, B), 0)
        cols = lax.broadcasted_iota(jnp.int32, (B, B), 1)
        diagonal = rows == cols
        five = jnp.where(diagonal, F32(5.0), F32(0.0))
        ridge = jnp.where(diagonal, F32(RIDGE), F32(0.0))
        sides = [(k, e) for k in owned for e in range(2)]
        stats = []
        for k in owned:
            grad = low(gbuf[k])
            turned = grad.T
            stats += [dot(grad, turned), dot(turned, grad)]
        current, factor, result = [], [], []
        for (k, e), stat in zip(sides, stats):
            fresh = DECAY * fbuf[k, e] + (1.0 - DECAY) * stat
            fbuf[k, e] = fresh
            ridged = fresh + ridge
            scale = jnp.sqrt(total(ridged * ridged) + NORM_EPS)
            current.append(ridged / scale)
            factor.append((five - current[-1]) * 0.25)
            result.append(low(factor[-1] / jnp.sqrt(jnp.sqrt(scale))))
        for turn in range(1, NEWTON):
            factor = [low(value) for value in factor]
            square = [low(dot(value, value)) for value in factor]
            fourth = [low(dot(value, value)) for value in square]
            current = [dot(value, low(old)) for value, old in zip(fourth, current)]
            factor = [(five - value) * 0.25 for value in current]
            result = [low(dot(old, low(value))) for old, value in zip(result, factor)]
        for (k, e), value in zip(sides, result):
            name = group * (2 * OWN) + 2 * k + e
            hits = total(jnp.where(listing[t] == name, F32(1.0), F32(0.0)))
            qbuf[k, e] = jnp.where(hits > 0.5, value, qbuf[k, e])

    def w_at(dx, dy, k):
        return wg.at[slot(dx, dy, c, k)]

    def share(dx, dy, k):
        ref = w_at(dx, dy, k)
        send(("d", dx, dy, k), ref, ref, sib)

    def gather_blocks():
        def ship(name, ref, dev):
            send(name, ref, ref, dev)

        for k in (1, 2, 0):
            finish_sum(0, k)
            wg[slot(0, 0, c, k)] = update(k)
            ship(("yo", k), w_at(0, 0, k), yp)
            ship(("r", k), w_at(0, 0, k), xr)
            ship(("l", k), w_at(0, 0, k), xl)
            share(0, 0, k)
        top, bottom = pl.ds(0, H), pl.ds(H, H)
        refresh(0, (1,))
        arrived(("r", 1), w_at(3, 0, 1), xl)
        share(3, 0, 1)
        arrived(("l", 1), w_at(1, 0, 1), xr)
        share(1, 0, 1)
        refresh(0, (2,))
        for k in (1, 2):
            arrived(("yo", k), w_at(0, 1, k), yp)
            ship(("rp", k), w_at(0, 1, k), xr)
            ship(("lp", k), w_at(0, 1, k), xl)
            share(0, 1, k)
        arrived(("r", 2), w_at(3, 0, 2), xl)
        share(3, 0, 2)
        arrived(("l", 2), w_at(1, 0, 2), xr)
        share(1, 0, 2)
        arrived(("r", 0), w_at(3, 0, 0), xl)
        ship("rh", w_at(3, 0, 0).at[top], xr)
        ship(("ya", "L"), w_at(3, 0, 0), yp)
        share(3, 0, 0)
        arrived(("l", 0), w_at(1, 0, 0), xr)
        ship("lh", w_at(1, 0, 0).at[bottom], xl)
        ship(("ya", "R"), w_at(1, 0, 0), yp)
        share(1, 0, 0)
        ship(("rf", 0), w_at(3, 0, 1), xr)
        ship(("lf", 0), w_at(1, 0, 2), xl)
        refresh(0, (0,))
        arrived(("yo", 0), w_at(0, 1, 0), yp)
        share(0, 1, 0)
        for k in (1, 2):
            arrived(("rp", k), w_at(3, 1, k), xl)
            if k == 1:
                ship(("rf", 1), w_at(3, 1, 1), xr)
            share(3, 1, k)
            arrived(("lp", k), w_at(1, 1, k), xr)
            if k == 2:
                ship(("lf", 1), w_at(1, 1, 2), xl)
            share(1, 1, k)
        arrived(("ya", "L"), w_at(3, 1, 0), yp)
        share(3, 1, 0)
        arrived("rh", w_at(2, 0, 0).at[top], xl)
        arrived("lh", w_at(2, 0, 0).at[bottom], xr)
        ship(("ya", "F"), w_at(2, 0, 0), yp)
        share(2, 0, 0)
        arrived(("ya", "R"), w_at(1, 1, 0), yp)
        share(1, 1, 0)
        for dy in range(2):
            arrived(("rf", dy), w_at(2, dy, 1), xl)
            share(2, dy, 1)
            arrived(("lf", dy), w_at(2, dy, 2), xr)
            share(2, dy, 2)
        arrived(("ya", "F"), w_at(2, 1, 0), yp)
        share(2, 1, 0)
        for dx, dy, k in ORDER:
            arrived(("d", dx, dy, k), wg.at[slot(dx, dy, 1 - c, k)], sib)

    load_x[0].wait()
    transpose(xraw, 0, 0)
    load_a.wait()
    gate(0, wait_weights, lambda i, j: wbuf[j * RB + i])
    arrived(("x", 0), xpeer.at[0], sib)
    transpose(xpeer, 0, 1)
    wait_dgate(0)

    def meanwhile():
        for k in range(OWN):
            wown[k] = wbuf[place[2, OWN * r + k]]
        load_x[1].wait()
        transpose(xraw, 1, 0)
        arrived(("x", 1), xpeer.at[1], sib)
        transpose(xpeer, 1, 1)
        load_f.wait()
        load_q.wait()

    reduce_blocks(0, meanwhile)
    gather_blocks()

    gate(1, lambda j: None, lambda i, j: wg[owner[0, i * CB + j]])
    wait_dgate(1)
    reduce_blocks(1, lambda: None)
    for ks in ((1, 2), (0,)):
        for k in ks:
            finish_sum(1, k)
            wout[0, k] = update(k)
        refresh(1, ks)
        for k in ks:
            for e in range(2):
                rout[0, k, e] = qbuf[k, e]
    for copy in started:
        copy.wait_send()


def deliver(weights, roots, wout, rout, held, insem, outsem):
    pieces = [(weights.at[0, k], wout.at[0, k]) for k in range(OWN)]
    pieces += [(roots.at[0, k, e], rout.at[0, k, e]) for k in range(OWN) for e in range(2)]
    incoming, outgoing = [], []
    for n, (src, dst) in enumerate(pieces):
        incoming.append(pltpu.make_async_copy(src, held.at[n], insem.at[n]))
        outgoing.append(pltpu.make_async_copy(held.at[n], dst, outsem.at[n]))
        incoming[n].start()
    for n in range(len(pieces)):
        incoming[n].wait()
        outgoing[n].start()
    for n in range(len(pieces)):
        outgoing[n].wait()


def body(features, grad_act, weights, owner_slot, factors, roots, helper_list):
    ids = jnp.arange(RB * CB, dtype=jnp.int32)
    rows, cols = ids // CB, ids % CB
    kinds = jnp.arange(3, dtype=jnp.int32)[:, None]
    wanted = jnp.where(kinds == 0, rows, jnp.where(kinds == 1, cols, cols * RB + rows))
    placing = owner_slot[0][None, :] == ids[:, None]
    place = jnp.sum(jnp.where(placing[None], wanted[:, None, :], 0), axis=2)
    listing = jnp.swapaxes(helper_list, 1, 2)
    tokens = features.shape[1]
    anywhere = pl.BlockSpec(memory_space=pl.ANY)
    scalars = pl.BlockSpec(memory_space=pltpu.SMEM)
    local = pl.BlockSpec(memory_space=pltpu.VMEM)
    block = (B, B)
    results = (
        jax.ShapeDtypeStruct((1, OWN) + block, BF16),
        jax.ShapeDtypeStruct((1, OWN, 2) + block, BF16),
    )
    made = pl.pallas_call(
        kernel,
        out_shape=results,
        in_specs=[scalars, scalars, local] + [anywhere] * 5,
        out_specs=(local, local),
        scratch_shapes=[
            pltpu.VMEM((2, tokens, RB * B), BF16),
            pltpu.VMEM((2, tokens, RB * B), BF16),
            pltpu.VMEM((RB, B, 2 * tokens), BF16),
            pltpu.VMEM((RB, B, 2 * tokens), BF16),
            pltpu.VMEM((CB * RB,) + block, BF16),
            pltpu.VMEM((2, tokens, CB * B), BF16),
            pltpu.VMEM((CB, 2 * tokens, B), BF16),
            pltpu.VMEM((CB, 2 * tokens, B), BF16),
            pltpu.VMEM((2, len(ORDER)) + block, BF16),
            pltpu.VMEM((RB * CB,) + block, BF16),
            pltpu.VMEM((OWN,) + block, BF16),
            pltpu.VMEM((OWN,) + block, F32),
            pltpu.VMEM((OWN, 2) + block, F32),
            pltpu.VMEM((OWN, 2) + block, BF16),
            pltpu.VMEM((2, 2, 2) + block, BF16),
            pltpu.VMEM((2, 2, 2) + block, BF16),
            pltpu.VMEM((2, 2, 2) + block, BF16),
            pltpu.VMEM((2, 4) + block, BF16),
            pltpu.VMEM((2, 2, H, B), BF16),
            pltpu.VMEM((2, 2, H, B), BF16),
            pltpu.VMEM((2, 2, H, B), BF16),
            pltpu.VMEM((2, 2) + block, BF16),
            pltpu.SemaphoreType.DMA((len(NAMES),)),
            pltpu.SemaphoreType.DMA((len(NAMES),)),
            pltpu.SemaphoreType.DMA((16,)),
        ],
        compiler_params=pltpu.CompilerParams(
            collective_id=0, has_side_effects=True, vmem_limit_bytes=60 * 1024 * 1024
        ),
    )(place, owner_slot, listing, features, grad_act, weights, factors, roots)
    return pl.pallas_call(
        deliver,
        out_shape=results,
        in_specs=[anywhere] * 2,
        out_specs=(anywhere, anywhere),
        scratch_shapes=[
            pltpu.VMEM((3 * OWN,) + block, BF16),
            pltpu.SemaphoreType.DMA((3 * OWN,)),
            pltpu.SemaphoreType.DMA((3 * OWN,)),
        ],
    )(*made)


def solution(mesh):
    return jax.shard_map(
        body,
        mesh=mesh,
        in_specs=(
            P(None, "rep", None),
            P(None, "rep", "blk"),
            P(None, "blk"),
            P("blk", None),
            P("blk", "rep", None, None, None),
            P("blk", "rep", None, None, None),
            P(),
        ),
        out_specs=(P("blk", "rep", None, None), P("blk", "rep", None, None, None)),
        check_vma=False,
    )
```

```python
import jax
import jax.numpy as jnp
from jax import lax
from jax.experimental import pallas as pl
from jax.experimental.pallas import tpu as pltpu
from jax.sharding import PartitionSpec as P

NEWTON = 3
RIDGE = 0.001
NORM_EPS = 1e-06
DECAY = 0.95
STEP_SIZE = 0.5

B = 256
H = B // 2
OWN = 3
RB = 8
CB = 6
XN = 4
F32 = jnp.float32
BF16 = jnp.bfloat16
MESH = pl.DeviceIdType.MESH

ORDER = (
    [(2, 1, 1), (2, 1, 2), (2, 1, 0), (2, 0, 1), (2, 0, 2)]
    + [(1, 1, 0), (3, 1, 0), (0, 1, 0)]
    + [(1, 1, 2), (3, 1, 1), (1, 1, 1), (3, 1, 2)]
    + [(1, 0, 2), (3, 0, 1), (1, 0, 1), (3, 0, 2)]
    + [(2, 0, 0), (1, 0, 0), (3, 0, 0), (0, 0, 0)]
    + [(0, 1, 1), (0, 1, 2), (0, 0, 1), (0, 0, 2)]
)
PLACE = {item: q for q, item in enumerate(ORDER)}


def transfer_names():
    names = [("x", 0), ("x", 1)]
    for t in range(2):
        names += [("D", t, j) for j in range(CB)]
        names += [("s1", t, way, dy) for way in range(2) for dy in range(2)]
        names += [("a1", t, dx) for dx in range(4)]
        names += [("in", t, way, dy) for way in range(2) for dy in range(2)]
        names += [("de", t, way, dy) for way in range(2) for dy in range(2)]
        names += [(kind, t, way) for kind in ("fa", "ia", "da") for way in range(2)]
        names += [("b2", t, k) for k in (1, 2)]
    names += [(kind, k) for kind in ("yo", "r", "l") for k in range(OWN)]
    names += [(kind, k) for kind in ("rp", "lp") for k in (1, 2)]
    names += [("ya", place) for place in "LRF"]
    names += ["rh", "lh"]
    names += [(kind, dy) for kind in ("rf", "lf") for dy in range(2)]
    names += [("d",) + item for item in ORDER]
    return {name: n for n, name in enumerate(names)}


NAMES = transfer_names()


def dot(first, second):
    return jnp.dot(first, second, preferred_element_type=F32)


def low(value):
    return value.astype(BF16)


def total(value):
    return jnp.sum(value, axis=(0, 1), keepdims=True)


def kernel(
    place, owner, listing, feat, act, wts, fac, rts,
    wout, rout,
    xraw, xpeer, xt0, xt1, wbuf, actb, own0, own1, other0, other1, pb, wg, wown, gbuf, fbuf, qbuf,
    fwdb, froml, fromr, ya, fwda, fromla, fromra, yb,
    ssem, rsem, lsem,
):
    xt, db = (xt0, xt1), ((own0, other0), (own1, other1))
    r = lax.axis_index("rep")
    group = lax.axis_index("blk")
    c = lax.rem(r, 2)
    x = lax.rem(r // 2, XN)
    y = r // (2 * XN)

    def rep_of(yy, xx, cc):
        return (yy * XN + xx) * 2 + cc

    def right_by(dx):
        return lax.rem(x + dx, XN)

    def y_of(dy):
        return y if dy == 0 else 1 - y

    def slot(dx, dy, cc, k):
        return OWN * rep_of(y_of(dy), right_by(dx), cc) + k

    sib = rep_of(y, x, 1 - c)
    yp = rep_of(1 - y, x, c)
    xr = rep_of(y, right_by(1), c)
    xl = rep_of(y, right_by(3), c)

    def load(n, src, dst):
        copy = pltpu.make_async_copy(src, dst, lsem.at[n])
        copy.start()
        return copy

    def wait_weights(j):
        columns = wbuf.at[pl.ds(j * RB, RB)]
        pltpu.make_async_copy(columns, columns, lsem.at[j]).wait()

    load_x = [load(CB, feat.at[0], xraw.at[0])]
    load_a = load(CB + 1, act.at[0], actb.at[0])
    for j in range(CB):
        for i in range(RB):
            load(j, wts.at[pl.ds(i * B, B), pl.ds(j * B, B)], wbuf.at[j * RB + i])
    load_x.append(load(CB + 2, feat.at[1], xraw.at[1]))
    load_b = load(CB + 5, act.at[1], actb.at[1])
    load_f = load(CB + 3, fac.at[0], fbuf)
    load_q = load(CB + 4, rts.at[0], qbuf)

    barrier = pltpu.get_barrier_semaphore()
    for partner in (sib, yp, xr, xl):
        pl.semaphore_signal(barrier, inc=1, device_id={"rep": partner}, device_id_type=MESH)
    pl.semaphore_wait(barrier, 4)

    started = []

    def remote(n, src, dst, dev):
        return pltpu.make_async_remote_copy(
            src_ref=src, dst_ref=dst, send_sem=ssem.at[n], recv_sem=rsem.at[n],
            device_id={"rep": dev}, device_id_type=MESH,
        )

    def send(name, src, dst, dev):
        copy = remote(NAMES[name], src, dst, dev)
        copy.start()
        started.append(copy)

    def arrived(name, ref, dev):
        remote(NAMES[name], ref, ref, dev).wait_recv()

    for t in range(2):
        send(("x", t), feat.at[t], xpeer.at[t], sib)

    def turn(src, t, half, i):
        cols = pl.ds(pl.multiple_of(i * B, B), B)
        xt[t][i, :, half * B:(half + 1) * B] = src[t, :, cols].T

    def transpose(src, t, half):
        def one(i, carry):
            turn(src, t, half, i)
            return carry
        lax.fori_loop(0, RB, one, 0)

    def gate(t, ready, block, beside):
        def pair(n, carry):
            columns = (2 * n, 2 * n + 1)
            values = []
            for j in columns:
                ready(j)
            for j in columns:
                value = dot(xraw[t, :, 0:B], block(0, j))
                for i in range(1, RB):
                    value = value + dot(xraw[t, :, i * B:(i + 1) * B], block(i, j))
                values.append(value)
            beside(n)
            for j, value in zip(columns, values):
                sigmoid = 1.0 / (1.0 + jnp.exp(-value))
                slope = sigmoid * (1.0 + value * (1.0 - sigmoid))
                cols = pl.ds(pl.multiple_of(j * B, B), B)
                db[t][0][j] = low(actb[t, :, cols].astype(F32) * slope)
            for j in columns:
                remote(
                    NAMES[("D", t, 0)] + j, db[t][0].at[j], db[t][1].at[j], sib
                ).start()
            return carry
        lax.fori_loop(0, CB // 2, pair, 0)
        for m, (dx, dy, k) in enumerate(ORDER[:2]):
            gbuf[1 + m] = half_product(t, slot(dx, dy, c, k), 0)

    def half_product(t, here, half):
        part = slice(half * B, (half + 1) * B)
        return dot(xt[t][place[0, here], :, part], db[t][half][place[1, here]])

    def wait_dgate(t):
        for j in range(CB):
            own, other = db[t][0].at[j], db[t][1].at[j]
            started.append(remote(NAMES[("D", t, j)], own, other, sib))
            arrived(("D", t, j), other, sib)

    def partial(t, at, here):
        pb[t, at] = low(half_product(t, here, 0) + half_product(t, here, 1))

    def partials(t, first, count, looped=False):
        slots = [slot(dx, dy, c, k) for dx, dy, k in ORDER[first:first + count]]
        if not looped:
            for m in range(count):
                partial(t, first + m, slots[m])
            return

        def one(n, carry):
            here = slots[0]
            for m in range(1, count):
                here = jnp.where(n == m, slots[m], here)
            partial(t, first + n, here)
            return carry
        lax.fori_loop(0, count, one, 0)

    def p(t, dx, dy, k):
        return pb.at[t, PLACE[(dx, dy, k)]]

    side = ((xr, 1, xl), (xl, 3, xr))
    land = (froml, fromr)
    halves = (pl.ds(0, H), pl.ds(H, H))
    land_a = (fromla, fromra)

    def reduce_blocks(t, between):
        def start(dy):
            for way in range(2):
                send(("s1", t, way, dy), p(t, 2, dy, 1 + way), fwdb.at[t, way, dy], side[way][0])

        def near(dy):
            for way in range(2):
                k = 2 - way
                send(("in", t, way, dy), p(t, side[way][1], dy, k), land[way].at[t, dy, k - 1], side[way][0])

        def across(dx):
            send(("a1", t, dx), p(t, dx, 1, 0), ya.at[t, dx], yp)

        def pass_on(dy):
            for way in range(2):
                k = 1 + way
                arrived(("s1", t, way, dy), fwdb.at[t, way, dy], side[way][2])
                mine = p(t, side[way][1], dy, k)
                mine[...] = low(mine[...].astype(F32) + fwdb[t, way, dy].astype(F32))
                send(("de", t, way, dy), mine, land[way].at[t, dy, k - 1], side[way][0])

        def add_y(dx):
            arrived(("a1", t, dx), ya.at[t, dx], yp)
            return p(t, dx, 0, 0)[...].astype(F32) + ya[t, dx].astype(F32)

        for m, (dx, dy, k) in enumerate(ORDER[:2]):
            pb[t, m] = low(gbuf[1 + m] + half_product(t, slot(dx, dy, c, k), 1))
        start(1)
        partials(t, 2, 1)
        across(2)
        partials(t, 3, 2)
        start(0)
        partials(t, 5, 3)
        for dx in (1, 3, 0):
            across(dx)
        partials(t, 8, 4)
        near(1)
        for first in (12, 16, 20):
            partials(t, first, 4, looped=True)
        between()
        pass_on(1)
        p(t, 2, 0, 0)[...] = low(add_y(2))
        for way in range(2):
            send(("fa", t, way), p(t, 2, 0, 0).at[halves[way]], fwda.at[t, way], side[way][0])
        near(0)
        pass_on(0)
        for way in range(2):
            dx = side[way][1]
            p(t, dx, 0, 0)[...] = low(add_y(dx))
            send(("ia", t, way), p(t, dx, 0, 0).at[halves[1 - way]], land_a[way].at[t, 1 - way], side[way][0])
        gbuf[0] = add_y(0)
        for k in (1, 2):
            p(t, 0, 1, k)[...] = low(summed(t, 1, k))
            send(("b2", t, k), p(t, 0, 1, k), yb.at[t, k - 1], yp)
        for way in range(2):
            arrived(("fa", t, way), fwda.at[t, way], side[way][2])
            mine = p(t, side[way][1], 0, 0).at[halves[way]]
            mine[...] = low(mine[...].astype(F32) + fwda[t, way].astype(F32))
            send(("da", t, way), mine, land_a[way].at[t, way], side[way][0])

    def summed(t, dy, k):
        for way in range(2):
            kind = "de" if k == 1 + way else "in"
            arrived((kind, t, way, dy), land[way].at[t, dy, k - 1], side[way][2])
        return (
            p(t, 0, dy, k)[...].astype(F32)
            + froml[t, dy, k - 1].astype(F32) + fromr[t, dy, k - 1].astype(F32)
        )

    def finish_sum(t, k):
        if k > 0:
            value = summed(t, 0, k)
            arrived(("b2", t, k), yb.at[t, k - 1], yp)
            gbuf[k] = value + yb[t, k - 1].astype(F32)
            return
        for way in range(2):
            arrived(("ia", t, way), land_a[way].at[t, 1 - way], side[way][2])
            arrived(("da", t, way), land_a[way].at[t, way], side[way][2])
        for half in range(2):
            rows = slice(half * H, (half + 1) * H)
            gbuf[0, rows, :] += fromla[t, half].astype(F32) + fromra[t, half].astype(F32)

    def update(k):
        grad = gbuf[k]
        left = low(dot(qbuf[k, 0], low(grad)))
        shaped = dot(left, qbuf[k, 1])
        grad_norm = jnp.sqrt(total(grad * grad) + NORM_EPS)
        shaped_norm = jnp.sqrt(total(shaped * shaped) + NORM_EPS)
        value = low(wown[k].astype(F32) - STEP_SIZE * (grad_norm / shaped_norm) * shaped)
        wown[k] = value
        return value

    def refresh(t, owned):
        rows = lax.broadcasted_iota(jnp.int32, (B, B), 0)
        cols = lax.broadcasted_iota(jnp.int32, (B, B), 1)
        diagonal = rows == cols
        five = jnp.where(diagonal, F32(5.0), F32(0.0))
        ridge = jnp.where(diagonal, F32(RIDGE), F32(0.0))
        sides = [(k, e) for k in owned for e in range(2)]
        stats = []
        for k in owned:
            grad = low(gbuf[k])
            turned = grad.T
            stats += [dot(grad, turned), dot(turned, grad)]
        current, factor, result = [], [], []
        for (k, e), stat in zip(sides, stats):
            fresh = DECAY * fbuf[k, e] + (1.0 - DECAY) * stat
            fbuf[k, e] = fresh
            ridged = fresh + ridge
            scale = jnp.sqrt(total(ridged * ridged) + NORM_EPS)
            current.append(ridged / scale)
            factor.append((five - current[-1]) * 0.25)
            result.append(low(factor[-1] / jnp.sqrt(jnp.sqrt(scale))))
        for turn in range(1, NEWTON):
            factor = [low(value) for value in factor]
            square = [low(dot(value, value)) for value in factor]
            fourth = [low(dot(value, value)) for value in square]
            current = [dot(value, low(old)) for value, old in zip(fourth, current)]
            factor = [(five - value) * 0.25 for value in current]
            result = [low(dot(old, low(value))) for old, value in zip(result, factor)]
        for (k, e), value in zip(sides, result):
            name = group * (2 * OWN) + 2 * k + e
            hits = total(jnp.where(listing[t] == name, F32(1.0), F32(0.0)))
            qbuf[k, e] = jnp.where(hits > 0.5, value, qbuf[k, e])

    def w_at(dx, dy, k):
        return wg.at[slot(dx, dy, c, k)]

    def share(dx, dy, k):
        ref = w_at(dx, dy, k)
        send(("d", dx, dy, k), ref, ref, sib)

    def gather_blocks():
        def ship(name, ref, dev):
            send(name, ref, ref, dev)

        for k in (1, 2, 0):
            finish_sum(0, k)
            wg[slot(0, 0, c, k)] = update(k)
            ship(("yo", k), w_at(0, 0, k), yp)
            ship(("r", k), w_at(0, 0, k), xr)
            ship(("l", k), w_at(0, 0, k), xl)
            share(0, 0, k)
        top, bottom = pl.ds(0, H), pl.ds(H, H)
        refresh(0, (1,))
        arrived(("r", 1), w_at(3, 0, 1), xl)
        share(3, 0, 1)
        arrived(("l", 1), w_at(1, 0, 1), xr)
        share(1, 0, 1)
        refresh(0, (2,))
        for k in (1, 2):
            arrived(("yo", k), w_at(0, 1, k), yp)
            ship(("rp", k), w_at(0, 1, k), xr)
            ship(("lp", k), w_at(0, 1, k), xl)
            share(0, 1, k)
        arrived(("r", 2), w_at(3, 0, 2), xl)
        share(3, 0, 2)
        arrived(("l", 2), w_at(1, 0, 2), xr)
        share(1, 0, 2)
        arrived(("r", 0), w_at(3, 0, 0), xl)
        ship("rh", w_at(3, 0, 0).at[top], xr)
        ship(("ya", "L"), w_at(3, 0, 0), yp)
        share(3, 0, 0)
        arrived(("l", 0), w_at(1, 0, 0), xr)
        ship("lh", w_at(1, 0, 0).at[bottom], xl)
        ship(("ya", "R"), w_at(1, 0, 0), yp)
        share(1, 0, 0)
        ship(("rf", 0), w_at(3, 0, 1), xr)
        ship(("lf", 0), w_at(1, 0, 2), xl)
        refresh(0, (0,))
        arrived(("yo", 0), w_at(0, 1, 0), yp)
        share(0, 1, 0)
        for k in (1, 2):
            arrived(("rp", k), w_at(3, 1, k), xl)
            if k == 1:
                ship(("rf", 1), w_at(3, 1, 1), xr)
            share(3, 1, k)
            arrived(("lp", k), w_at(1, 1, k), xr)
            if k == 2:
                ship(("lf", 1), w_at(1, 1, 2), xl)
            share(1, 1, k)
        arrived(("ya", "L"), w_at(3, 1, 0), yp)
        share(3, 1, 0)
        arrived("rh", w_at(2, 0, 0).at[top], xl)
        arrived("lh", w_at(2, 0, 0).at[bottom], xr)
        ship(("ya", "F"), w_at(2, 0, 0), yp)
        share(2, 0, 0)
        arrived(("ya", "R"), w_at(1, 1, 0), yp)
        share(1, 1, 0)
        for dy in range(2):
            arrived(("rf", dy), w_at(2, dy, 1), xl)
            share(2, dy, 1)
            arrived(("lf", dy), w_at(2, dy, 2), xr)
            share(2, dy, 2)
        arrived(("ya", "F"), w_at(2, 1, 0), yp)
        share(2, 1, 0)
        for dx, dy, k in ORDER:
            arrived(("d", dx, dy, k), wg.at[slot(dx, dy, 1 - c, k)], sib)

    load_x[0].wait()
    load_a.wait()

    def turn_own(n):
        for m in range(3):
            turn(xraw, 0, 0, jnp.minimum(3 * n + m, RB - 1))

    gate(0, wait_weights, lambda i, j: wbuf[j * RB + i], turn_own)
    arrived(("x", 0), xpeer.at[0], sib)
    transpose(xpeer, 0, 1)
    wait_dgate(0)

    def meanwhile():
        for k in range(OWN):
            wown[k] = wbuf[place[2, OWN * r + k]]
        load_x[1].wait()
        transpose(xraw, 1, 0)
        arrived(("x", 1), xpeer.at[1], sib)
        transpose(xpeer, 1, 1)
        load_b.wait()
        load_f.wait()
        load_q.wait()

    reduce_blocks(0, meanwhile)
    gather_blocks()

    gate(1, lambda j: None, lambda i, j: wg[owner[0, i * CB + j]], lambda n: None)
    wait_dgate(1)
    reduce_blocks(1, lambda: None)
    for ks in ((1, 2), (0,)):
        for k in ks:
            finish_sum(1, k)
            wout[0, k] = update(k)
        refresh(1, ks)
        for k in ks:
            for e in range(2):
                rout[0, k, e] = qbuf[k, e]
    for copy in started:
        copy.wait_send()


def deliver(weights, roots, wout, rout, held, insem, outsem):
    pieces = [(weights.at[0, k], wout.at[0, k]) for k in range(OWN)]
    pieces += [(roots.at[0, k, e], rout.at[0, k, e]) for k in range(OWN) for e in range(2)]
    incoming, outgoing = [], []
    for n, (src, dst) in enumerate(pieces):
        incoming.append(pltpu.make_async_copy(src, held.at[n], insem.at[n]))
        outgoing.append(pltpu.make_async_copy(held.at[n], dst, outsem.at[n]))
        incoming[n].start()
    for n in range(len(pieces)):
        incoming[n].wait()
        outgoing[n].start()
    for n in range(len(pieces)):
        outgoing[n].wait()


def body(features, grad_act, weights, owner_slot, factors, roots, helper_list):
    ids = jnp.arange(RB * CB, dtype=jnp.int32)
    rows, cols = ids // CB, ids % CB
    kinds = jnp.arange(3, dtype=jnp.int32)[:, None]
    wanted = jnp.where(kinds == 0, rows, jnp.where(kinds == 1, cols, cols * RB + rows))
    placing = owner_slot[0][None, :] == ids[:, None]
    place = jnp.sum(jnp.where(placing[None], wanted[:, None, :], 0), axis=2)
    listing = jnp.swapaxes(helper_list, 1, 2)
    tokens = features.shape[1]
    anywhere = pl.BlockSpec(memory_space=pl.ANY)
    scalars = pl.BlockSpec(memory_space=pltpu.SMEM)
    local = pl.BlockSpec(memory_space=pltpu.VMEM)
    block = (B, B)
    results = (
        jax.ShapeDtypeStruct((1, OWN) + block, BF16),
        jax.ShapeDtypeStruct((1, OWN, 2) + block, BF16),
    )
    made = pl.pallas_call(
        kernel,
        out_shape=results,
        in_specs=[scalars, scalars, local] + [anywhere] * 5,
        out_specs=(local, local),
        scratch_shapes=[
            pltpu.VMEM((2, tokens, RB * B), BF16),
            pltpu.VMEM((2, tokens, RB * B), BF16),
            pltpu.VMEM((RB, B, 2 * tokens), BF16),
            pltpu.VMEM((RB, B, 2 * tokens), BF16),
            pltpu.VMEM((CB * RB,) + block, BF16),
            pltpu.VMEM((2, tokens, CB * B), BF16),
            pltpu.VMEM((CB, tokens, B), BF16),
            pltpu.VMEM((CB, tokens, B), BF16),
            pltpu.VMEM((CB, tokens, B), BF16),
            pltpu.VMEM((CB, tokens, B), BF16),
            pltpu.VMEM((2, len(ORDER)) + block, BF16),
            pltpu.VMEM((RB * CB,) + block, BF16),
            pltpu.VMEM((OWN,) + block, BF16),
            pltpu.VMEM((OWN,) + block, F32),
            pltpu.VMEM((OWN, 2) + block, F32),
            pltpu.VMEM((OWN, 2) + block, BF16),
            pltpu.VMEM((2, 2, 2) + block, BF16),
            pltpu.VMEM((2, 2, 2) + block, BF16),
            pltpu.VMEM((2, 2, 2) + block, BF16),
            pltpu.VMEM((2, 4) + block, BF16),
            pltpu.VMEM((2, 2, H, B), BF16),
            pltpu.VMEM((2, 2, H, B), BF16),
            pltpu.VMEM((2, 2, H, B), BF16),
            pltpu.VMEM((2, 2) + block, BF16),
            pltpu.SemaphoreType.DMA((len(NAMES),)),
            pltpu.SemaphoreType.DMA((len(NAMES),)),
            pltpu.SemaphoreType.DMA((16,)),
        ],
        compiler_params=pltpu.CompilerParams(
            collective_id=0, has_side_effects=True, vmem_limit_bytes=60 * 1024 * 1024
        ),
    )(place, owner_slot, listing, features, grad_act, weights, factors, roots)
    return pl.pallas_call(
        deliver,
        out_shape=results,
        in_specs=[anywhere] * 2,
        out_specs=(anywhere, anywhere),
        scratch_shapes=[
            pltpu.VMEM((3 * OWN,) + block, BF16),
            pltpu.SemaphoreType.DMA((3 * OWN,)),
            pltpu.SemaphoreType.DMA((3 * OWN,)),
        ],
    )(*made)


def solution(mesh):
    return jax.shard_map(
        body,
        mesh=mesh,
        in_specs=(
            P(None, "rep", None),
            P(None, "rep", "blk"),
            P(None, "blk"),
            P("blk", None),
            P("blk", "rep", None, None, None),
            P("blk", "rep", None, None, None),
            P(),
        ),
        out_specs=(P("blk", "rep", None, None), P("blk", "rep", None, None, None)),
        check_vma=False,
    )
```

```python
import jax
import jax.numpy as jnp
from jax import lax
from jax.experimental import pallas as pl
from jax.experimental.pallas import tpu as pltpu
from jax.sharding import PartitionSpec as P

NEWTON = 3
RIDGE = 0.001
NORM_EPS = 1e-06
DECAY = 0.95
STEP_SIZE = 0.5

B = 256
S = 80
RA = B + S
R0 = 240
PIECES = {"0": (0, 0, B), "1a": (1, 0, S), "1b": (1, S, B - S), "2": (2, 0, B)}
OWN = 3
RB = 8
CB = 6
XN = 4
F32 = jnp.float32
BF16 = jnp.bfloat16
MESH = pl.DeviceIdType.MESH

ORDER = (
    [(2, 1, 1), (2, 1, 2), (2, 1, 0), (2, 0, 1), (2, 0, 2)]
    + [(1, 1, 0), (1, 1, 1), (3, 1, 0), (3, 1, 1), (1, 1, 2)]
    + [(0, 1, 0), (0, 1, 1), (3, 1, 2)]
    + [(1, 0, 2), (3, 0, 1), (1, 0, 1), (3, 0, 2)]
    + [(2, 0, 0), (1, 0, 0), (3, 0, 0), (0, 0, 0)]
    + [(0, 1, 2), (0, 0, 1), (0, 0, 2)]
)
PLACE = {item: q for q, item in enumerate(ORDER)}


def transfer_names():
    names = [("x", 0), ("x", 1)]
    for t in range(2):
        names += [("D", t, j) for j in range(CB)]
        names += [("s1", t, way, dy) for way in range(2) for dy in range(2)]
        names += [("a1", t, dx) for dx in range(4)]
        names += [("in", t, way, dy) for way in range(2) for dy in range(2)]
        names += [("de", t, way, dy) for way in range(2) for dy in range(2)]
        names += [(kind, t, way) for kind in ("fa", "ia", "da") for way in range(2)]
        names += [("b2", t, k) for k in (1, 2)]
    names += [(kind, piece) for kind in ("yo", "r", "l") for piece in PIECES]
    names += [(kind, piece) for kind in ("rp", "lp") for piece in ("2", "1b")]
    names += [("ya", place, piece) for place in "LRF" for piece in ("0", "1a")]
    names += ["rh", "lh0", "lh1"]
    names += [(kind, dy) for kind in ("rf", "lf") for dy in range(2)]
    names += [("d", dx, dy, piece) for dx in range(XN) for dy in range(2) for piece in PIECES]
    return {name: n for n, name in enumerate(names)}


NAMES = transfer_names()


def dot(first, second):
    return jnp.dot(first, second, preferred_element_type=F32)


def low(value):
    return value.astype(BF16)


def total(value):
    return jnp.sum(value, axis=(0, 1), keepdims=True)


def kernel(
    place, owner, listing, feat, act, wts, fac, rts,
    wout, rout,
    xraw, xpeer, xt0, xt1, wbuf, actb, own0, own1, other0, other1, pa, pb, wg, wown, ga, gbuf, fbuf, qbuf,
    fwdb, froml, fromr, ya, fwda, fromla, fromra, yb,
    ssem, rsem, lsem,
):
    xt, db = (xt0, xt1), ((own0, other0), (own1, other1))
    r = lax.axis_index("rep")
    group = lax.axis_index("blk")
    c = lax.rem(r, 2)
    x = lax.rem(r // 2, XN)
    y = r // (2 * XN)

    def rep_of(yy, xx, cc):
        return (yy * XN + xx) * 2 + cc

    def right_by(dx):
        return lax.rem(x + dx, XN)

    def y_of(dy):
        return y if dy == 0 else 1 - y

    def slot(dx, dy, cc, k):
        return OWN * rep_of(y_of(dy), right_by(dx), cc) + k

    sib = rep_of(y, x, 1 - c)
    yp = rep_of(1 - y, x, c)
    xr = rep_of(y, right_by(1), c)
    xl = rep_of(y, right_by(3), c)

    def load(n, src, dst):
        copy = pltpu.make_async_copy(src, dst, lsem.at[n])
        copy.start()
        return copy

    def wait_weights(j):
        columns = wbuf.at[pl.ds(j * RB, RB)]
        pltpu.make_async_copy(columns, columns, lsem.at[j]).wait()

    load_x = [load(CB, feat.at[0], xraw.at[0])]
    load_a = load(CB + 1, act.at[0], actb.at[0])
    for j in range(CB):
        for i in range(RB):
            load(j, wts.at[pl.ds(i * B, B), pl.ds(j * B, B)], wbuf.at[j * RB + i])
    load_x.append(load(CB + 2, feat.at[1], xraw.at[1]))
    load_b = load(CB + 5, act.at[1], actb.at[1])
    load_f = load(CB + 3, fac.at[0], fbuf)
    load_q = load(CB + 4, rts.at[0], qbuf)

    barrier = pltpu.get_barrier_semaphore()
    for partner in (sib, yp, xr, xl):
        pl.semaphore_signal(barrier, inc=1, device_id={"rep": partner}, device_id_type=MESH)
    pl.semaphore_wait(barrier, 4)

    started = []

    def remote(n, src, dst, dev):
        return pltpu.make_async_remote_copy(
            src_ref=src, dst_ref=dst, send_sem=ssem.at[n], recv_sem=rsem.at[n],
            device_id={"rep": dev}, device_id_type=MESH,
        )

    def send(name, src, dst, dev):
        copy = remote(NAMES[name], src, dst, dev)
        copy.start()
        started.append(copy)

    def arrived(name, ref, dev):
        remote(NAMES[name], ref, ref, dev).wait_recv()

    for t in range(2):
        send(("x", t), feat.at[t], xpeer.at[t], sib)

    def turn(src, t, half, i):
        cols = pl.ds(pl.multiple_of(i * B, B), B)
        xt[t][i, :, half * B:(half + 1) * B] = src[t, :, cols].T

    def transpose(src, t, half):
        def one(i, carry):
            turn(src, t, half, i)
            return carry
        lax.fori_loop(0, RB, one, 0)

    def gate(t, ready, block, beside):
        def pair(n, carry):
            columns = (2 * n, 2 * n + 1)
            values = []
            for j in columns:
                ready(j)
            for j in columns:
                value = dot(xraw[t, :, 0:B], block(0, j))
                for i in range(1, RB):
                    value = value + dot(xraw[t, :, i * B:(i + 1) * B], block(i, j))
                values.append(value)
            beside(n)
            for j, value in zip(columns, values):
                sigmoid = 1.0 / (1.0 + jnp.exp(-value))
                slope = sigmoid * (1.0 + value * (1.0 - sigmoid))
                cols = pl.ds(pl.multiple_of(j * B, B), B)
                db[t][0][j] = low(actb[t, :, cols].astype(F32) * slope)
            for j in columns:
                remote(
                    NAMES[("D", t, 0)] + j, db[t][0].at[j], db[t][1].at[j], sib
                ).start()
            return carry
        lax.fori_loop(0, CB // 2, pair, 0)
        for m, (dx, dy, k) in enumerate(ORDER[:2]):
            gbuf[1 + m] = half_product(t, slot(dx, dy, c, k), 0)

    def half_product(t, here, half):
        part = slice(half * B, (half + 1) * B)
        return dot(xt[t][place[0, here], :, part], db[t][half][place[1, here]])

    def wait_dgate(t):
        for j in range(CB):
            own, other = db[t][0].at[j], db[t][1].at[j]
            started.append(remote(NAMES[("D", t, j)], own, other, sib))
            arrived(("D", t, j), other, sib)

    def keep(t, at, value):
        dx, dy, k = ORDER[at]
        value = low(value)
        if k == 0:
            pa[t, 2 * dx + dy, 0:B, :] = value
        elif k == 1:
            pa[t, 2 * dx + dy, B:RA, :] = value[:S]
            pb[t, at, S:B, :] = value[S:]
        else:
            pb[t, at] = value

    def partials(t, first, count):
        for at in range(first, first + count):
            dx, dy, k = ORDER[at]
            here = slot(dx, dy, c, k)
            keep(t, at, half_product(t, here, 0) + half_product(t, here, 1))

    def rows_of(k):
        return pl.ds(S, B - S) if k == 1 else pl.ds(0, B)

    def p(t, dx, dy, k):
        return pb.at[t, PLACE[(dx, dy, k)], rows_of(k)]

    def first(t, dx, dy):
        return pa.at[t, 2 * dx + dy]

    side = ((xr, 1, xl), (xl, 3, xr))
    land = (froml, fromr)
    halves = (pl.ds(0, R0), pl.ds(R0, RA - R0))
    heads = (pl.ds(0, R0), pl.ds(0, RA - R0))
    land_a = (fromla, fromra)

    def reduce_blocks(t, between):
        def start(dy):
            for way in range(2):
                k = 1 + way
                send(("s1", t, way, dy), p(t, 2, dy, k), fwdb.at[t, way, dy, rows_of(k)], side[way][0])

        def near(dy):
            for way in range(2):
                k = 2 - way
                send(
                    ("in", t, way, dy), p(t, side[way][1], dy, k),
                    land[way].at[t, dy, k - 1, rows_of(k)], side[way][0],
                )

        def across(dx):
            send(("a1", t, dx), first(t, dx, 1), ya.at[t, dx], yp)

        def pass_on(dy):
            for way in range(2):
                k = 1 + way
                came = fwdb.at[t, way, dy, rows_of(k)]
                arrived(("s1", t, way, dy), came, side[way][2])
                mine = p(t, side[way][1], dy, k)
                mine[...] = low(mine[...].astype(F32) + came[...].astype(F32))
                send(("de", t, way, dy), mine, land[way].at[t, dy, k - 1, rows_of(k)], side[way][0])

        def add_y(dx):
            arrived(("a1", t, dx), ya.at[t, dx], yp)
            return first(t, dx, 0)[...].astype(F32) + ya[t, dx].astype(F32)

        for m, (dx, dy, k) in enumerate(ORDER[:2]):
            keep(t, m, gbuf[1 + m] + half_product(t, slot(dx, dy, c, k), 1))
        start(1)
        partials(t, 2, 1)
        across(2)
        partials(t, 3, 2)
        start(0)
        partials(t, 5, 2)
        across(1)
        partials(t, 7, 2)
        across(3)
        partials(t, 9, 1)
        near(1)
        partials(t, 10, 2)
        across(0)
        partials(t, 12, 12)
        between()
        pass_on(1)
        first(t, 2, 0)[...] = low(add_y(2))
        for way in range(2):
            send(("fa", t, way), first(t, 2, 0).at[halves[way]], fwda.at[t, way, heads[way]], side[way][0])
        near(0)
        pass_on(0)
        for way in range(2):
            dx = side[way][1]
            first(t, dx, 0)[...] = low(add_y(dx))
            half = halves[1 - way]
            send(("ia", t, way), first(t, dx, 0).at[half], land_a[way].at[t, half], side[way][0])
        ga[...] = add_y(0)
        for k in (2, 1):
            p(t, 0, 1, k)[...] = low(summed(t, 1, k))
            send(("b2", t, k), p(t, 0, 1, k), yb.at[t, k - 1, rows_of(k)], yp)
        for way in range(2):
            came = fwda.at[t, way, heads[way]]
            arrived(("fa", t, way), came, side[way][2])
            mine = first(t, side[way][1], 0).at[halves[way]]
            mine[...] = low(mine[...].astype(F32) + came[...].astype(F32))
            send(("da", t, way), mine, land_a[way].at[t, halves[way]], side[way][0])

    def summed(t, dy, k):
        value = p(t, 0, dy, k)[...].astype(F32)
        for way in range(2):
            kind = "de" if k == 1 + way else "in"
            came = land[way].at[t, dy, k - 1, rows_of(k)]
            arrived((kind, t, way, dy), came, side[way][2])
            value = value + came[...].astype(F32)
        return value

    def finish_second(t, k):
        value = summed(t, 0, k)
        came = yb.at[t, k - 1, rows_of(k)]
        arrived(("b2", t, k), came, yp)
        gbuf[k, S if k == 1 else 0:B, :] = value + came[...].astype(F32)

    def finish_first(t):
        for way in range(2):
            for kind, half in (("ia", halves[1 - way]), ("da", halves[way])):
                arrived((kind, t, way), land_a[way].at[t, half], side[way][2])
        value = ga[...] + fromla[t].astype(F32) + fromra[t].astype(F32)
        gbuf[0] = value[:B]
        gbuf[1, 0:S, :] = value[B:]

    def update(k):
        grad = gbuf[k]
        left = low(dot(qbuf[k, 0], low(grad)))
        shaped = dot(left, qbuf[k, 1])
        grad_norm = jnp.sqrt(total(grad * grad) + NORM_EPS)
        shaped_norm = jnp.sqrt(total(shaped * shaped) + NORM_EPS)
        value = low(wown[k].astype(F32) - STEP_SIZE * (grad_norm / shaped_norm) * shaped)
        wown[k] = value
        return value

    def refresh(t, owned):
        rows = lax.broadcasted_iota(jnp.int32, (B, B), 0)
        cols = lax.broadcasted_iota(jnp.int32, (B, B), 1)
        diagonal = rows == cols
        five = jnp.where(diagonal, F32(5.0), F32(0.0))
        ridge = jnp.where(diagonal, F32(RIDGE), F32(0.0))
        sides = [(k, e) for k in owned for e in range(2)]
        stats = []
        for k in owned:
            grad = low(gbuf[k])
            turned = grad.T
            stats += [dot(grad, turned), dot(turned, grad)]
        current, factor, result = [], [], []
        for (k, e), stat in zip(sides, stats):
            fresh = DECAY * fbuf[k, e] + (1.0 - DECAY) * stat
            fbuf[k, e] = fresh
            ridged = fresh + ridge
            scale = jnp.sqrt(total(ridged * ridged) + NORM_EPS)
            current.append(ridged / scale)
            factor.append((five - current[-1]) * 0.25)
            result.append(low(factor[-1] / jnp.sqrt(jnp.sqrt(scale))))
        for turn in range(1, NEWTON):
            factor = [low(value) for value in factor]
            square = [low(dot(value, value)) for value in factor]
            fourth = [low(dot(value, value)) for value in square]
            current = [dot(value, low(old)) for value, old in zip(fourth, current)]
            factor = [(five - value) * 0.25 for value in current]
            result = [low(dot(old, low(value))) for old, value in zip(result, factor)]
        for (k, e), value in zip(sides, result):
            name = group * (2 * OWN) + 2 * k + e
            hits = total(jnp.where(listing[t] == name, F32(1.0), F32(0.0)))
            qbuf[k, e] = jnp.where(hits > 0.5, value, qbuf[k, e])

    def w_at(dx, dy, piece):
        k, begin, rows = PIECES[piece]
        return wg.at[slot(dx, dy, c, k), pl.ds(begin, rows)]

    def share(dx, dy, piece):
        ref = w_at(dx, dy, piece)
        send(("d", dx, dy, piece), ref, ref, sib)

    def gather_blocks():
        def ship(name, ref, dev):
            send(name, ref, ref, dev)

        def spread(piece):
            ref = w_at(0, 0, piece)
            ship(("yo", piece), ref, yp)
            ship(("r", piece), ref, xr)
            ship(("l", piece), ref, xl)
            share(0, 0, piece)

        def renew(k):
            wg[slot(0, 0, c, k)] = update(k)

        def expect(name, dx, dy, piece, dev):
            arrived(name, w_at(dx, dy, piece), dev)
            share(dx, dy, piece)

        finish_second(0, 2)
        renew(2)
        spread("2")
        finish_second(0, 1)
        finish_first(0)
        renew(1)
        spread("1b")
        renew(0)
        spread("0")
        spread("1a")
        refresh(0, (2,))
        expect(("r", "2"), 3, 0, "2", xl)
        expect(("l", "2"), 1, 0, "2", xr)
        refresh(0, (1,))
        for piece in ("2", "1b"):
            expect(("yo", piece), 0, 1, piece, yp)
            ship(("rp", piece), w_at(0, 1, piece), xr)
            ship(("lp", piece), w_at(0, 1, piece), xl)
        expect(("r", "1b"), 3, 0, "1b", xl)
        expect(("l", "1b"), 1, 0, "1b", xr)
        top, bottom = pl.ds(0, R0), pl.ds(R0, B - R0)
        expect(("r", "0"), 3, 0, "0", xl)
        ship("rh", wg.at[slot(3, 0, c, 0), top], xr)
        expect(("l", "0"), 1, 0, "0", xr)
        ship("lh0", wg.at[slot(1, 0, c, 0), bottom], xl)
        ship(("ya", "L", "0"), w_at(3, 0, "0"), yp)
        ship(("ya", "R", "0"), w_at(1, 0, "0"), yp)
        expect(("r", "1a"), 3, 0, "1a", xl)
        expect(("l", "1a"), 1, 0, "1a", xr)
        ship("lh1", w_at(1, 0, "1a"), xl)
        ship(("ya", "L", "1a"), w_at(3, 0, "1a"), yp)
        ship(("ya", "R", "1a"), w_at(1, 0, "1a"), yp)
        ship(("rf", 0), w_at(3, 0, "1b"), xr)
        ship(("lf", 0), w_at(1, 0, "2"), xl)
        refresh(0, (0,))
        for piece in ("0", "1a"):
            expect(("yo", piece), 0, 1, piece, yp)
        for piece in ("2", "1b"):
            expect(("rp", piece), 3, 1, piece, xl)
            if piece == "1b":
                ship(("rf", 1), w_at(3, 1, piece), xr)
            expect(("lp", piece), 1, 1, piece, xr)
            if piece == "2":
                ship(("lf", 1), w_at(1, 1, piece), xl)
        expect(("ya", "L", "0"), 3, 1, "0", yp)
        arrived("rh", wg.at[slot(2, 0, c, 0), top], xl)
        arrived("lh0", wg.at[slot(2, 0, c, 0), bottom], xr)
        ship(("ya", "F", "0"), w_at(2, 0, "0"), yp)
        share(2, 0, "0")
        expect("lh1", 2, 0, "1a", xr)
        ship(("ya", "F", "1a"), w_at(2, 0, "1a"), yp)
        expect(("ya", "R", "0"), 1, 1, "0", yp)
        expect(("ya", "L", "1a"), 3, 1, "1a", yp)
        expect(("ya", "R", "1a"), 1, 1, "1a", yp)
        for dy in range(2):
            expect(("rf", dy), 2, dy, "1b", xl)
            expect(("lf", dy), 2, dy, "2", xr)
        for piece in ("0", "1a"):
            expect(("ya", "F", piece), 2, 1, piece, yp)
        for dx in range(XN):
            for dy in range(2):
                for piece, (k, begin, rows) in PIECES.items():
                    ref = wg.at[slot(dx, dy, 1 - c, k), pl.ds(begin, rows)]
                    arrived(("d", dx, dy, piece), ref, sib)

    load_x[0].wait()
    load_a.wait()

    def turn_own(n):
        for m in range(3):
            turn(xraw, 0, 0, jnp.minimum(3 * n + m, RB - 1))

    gate(0, wait_weights, lambda i, j: wbuf[j * RB + i], turn_own)
    arrived(("x", 0), xpeer.at[0], sib)
    transpose(xpeer, 0, 1)
    wait_dgate(0)

    def meanwhile():
        for k in range(OWN):
            wown[k] = wbuf[place[2, OWN * r + k]]
        load_x[1].wait()
        transpose(xraw, 1, 0)
        arrived(("x", 1), xpeer.at[1], sib)
        transpose(xpeer, 1, 1)
        load_b.wait()
        load_f.wait()
        load_q.wait()

    reduce_blocks(0, meanwhile)
    gather_blocks()

    gate(1, lambda j: None, lambda i, j: wg[owner[0, i * CB + j]], lambda n: None)
    wait_dgate(1)
    reduce_blocks(1, lambda: None)
    def conclude(ks):
        for k in ks:
            wout[0, k] = update(k)
        refresh(1, ks)
        for k in ks:
            for e in range(2):
                rout[0, k, e] = qbuf[k, e]

    finish_second(1, 2)
    conclude((2,))
    finish_second(1, 1)
    finish_first(1)
    conclude((1, 0))
    for copy in started:
        copy.wait_send()


def deliver(weights, roots, wout, rout, held, insem, outsem):
    pieces = [(weights.at[0, k], wout.at[0, k]) for k in range(OWN)]
    pieces += [(roots.at[0, k, e], rout.at[0, k, e]) for k in range(OWN) for e in range(2)]
    incoming, outgoing = [], []
    for n, (src, dst) in enumerate(pieces):
        incoming.append(pltpu.make_async_copy(src, held.at[n], insem.at[n]))
        outgoing.append(pltpu.make_async_copy(held.at[n], dst, outsem.at[n]))
        incoming[n].start()
    for n in range(len(pieces)):
        incoming[n].wait()
        outgoing[n].start()
    for n in range(len(pieces)):
        outgoing[n].wait()


def body(features, grad_act, weights, owner_slot, factors, roots, helper_list):
    ids = jnp.arange(RB * CB, dtype=jnp.int32)
    rows, cols = ids // CB, ids % CB
    kinds = jnp.arange(3, dtype=jnp.int32)[:, None]
    wanted = jnp.where(kinds == 0, rows, jnp.where(kinds == 1, cols, cols * RB + rows))
    placing = owner_slot[0][None, :] == ids[:, None]
    place = jnp.sum(jnp.where(placing[None], wanted[:, None, :], 0), axis=2)
    listing = jnp.swapaxes(helper_list, 1, 2)
    tokens = features.shape[1]
    anywhere = pl.BlockSpec(memory_space=pl.ANY)
    scalars = pl.BlockSpec(memory_space=pltpu.SMEM)
    local = pl.BlockSpec(memory_space=pltpu.VMEM)
    block = (B, B)
    results = (
        jax.ShapeDtypeStruct((1, OWN) + block, BF16),
        jax.ShapeDtypeStruct((1, OWN, 2) + block, BF16),
    )
    made = pl.pallas_call(
        kernel,
        out_shape=results,
        in_specs=[scalars, scalars, local] + [anywhere] * 5,
        out_specs=(local, local),
        scratch_shapes=[
            pltpu.VMEM((2, tokens, RB * B), BF16),
            pltpu.VMEM((2, tokens, RB * B), BF16),
            pltpu.VMEM((RB, B, 2 * tokens), BF16),
            pltpu.VMEM((RB, B, 2 * tokens), BF16),
            pltpu.VMEM((CB * RB,) + block, BF16),
            pltpu.VMEM((2, tokens, CB * B), BF16),
            pltpu.VMEM((CB, tokens, B), BF16),
            pltpu.VMEM((CB, tokens, B), BF16),
            pltpu.VMEM((CB, tokens, B), BF16),
            pltpu.VMEM((CB, tokens, B), BF16),
            pltpu.VMEM((2, 2 * XN, RA, B), BF16),
            pltpu.VMEM((2, len(ORDER)) + block, BF16),
            pltpu.VMEM((RB * CB,) + block, BF16),
            pltpu.VMEM((OWN,) + block, BF16),
            pltpu.VMEM((RA, B), F32),
            pltpu.VMEM((OWN,) + block, F32),
            pltpu.VMEM((OWN, 2) + block, F32),
            pltpu.VMEM((OWN, 2) + block, BF16),
            pltpu.VMEM((2, 2, 2) + block, BF16),
            pltpu.VMEM((2, 2, 2) + block, BF16),
            pltpu.VMEM((2, 2, 2) + block, BF16),
            pltpu.VMEM((2, XN, RA, B), BF16),
            pltpu.VMEM((2, 2, R0, B), BF16),
            pltpu.VMEM((2, RA, B), BF16),
            pltpu.VMEM((2, RA, B), BF16),
            pltpu.VMEM((2, 2) + block, BF16),
            pltpu.SemaphoreType.DMA((len(NAMES),)),
            pltpu.SemaphoreType.DMA((len(NAMES),)),
            pltpu.SemaphoreType.DMA((16,)),
        ],
        compiler_params=pltpu.CompilerParams(
            collective_id=0, has_side_effects=True, vmem_limit_bytes=60 * 1024 * 1024
        ),
    )(place, owner_slot, listing, features, grad_act, weights, factors, roots)
    return pl.pallas_call(
        deliver,
        out_shape=results,
        in_specs=[anywhere] * 2,
        out_specs=(anywhere, anywhere),
        scratch_shapes=[
            pltpu.VMEM((3 * OWN,) + block, BF16),
            pltpu.SemaphoreType.DMA((3 * OWN,)),
            pltpu.SemaphoreType.DMA((3 * OWN,)),
        ],
    )(*made)


def solution(mesh):
    return jax.shard_map(
        body,
        mesh=mesh,
        in_specs=(
            P(None, "rep", None),
            P(None, "rep", "blk"),
            P(None, "blk"),
            P("blk", None),
            P("blk", "rep", None, None, None),
            P("blk", "rep", None, None, None),
            P(),
        ),
        out_specs=(P("blk", "rep", None, None), P("blk", "rep", None, None, None)),
        check_vma=False,
    )
```

```python
import jax
import jax.numpy as jnp
from jax import lax
from jax.experimental import pallas as pl
from jax.experimental.pallas import tpu as pltpu
from jax.sharding import PartitionSpec as P

NEWTON = 3
RIDGE = 0.001
NORM_EPS = 1e-06
DECAY = 0.95
STEP_SIZE = 0.5

B = 256
S = 80
RA = B + S
R0 = 240
PIECES = {"0": (0, 0, B), "1a": (1, 0, S), "1b": (1, S, B - S), "2": (2, 0, B)}
OWN = 3
RB = 8
CB = 6
XN = 4
F32 = jnp.float32
BF16 = jnp.bfloat16
MESH = pl.DeviceIdType.MESH

ORDER = (
    [(2, 1, 1), (2, 1, 2), (2, 1, 0), (2, 0, 1), (2, 0, 2)]
    + [(1, 1, 0), (1, 1, 1), (3, 1, 0), (3, 1, 1), (1, 1, 2)]
    + [(0, 1, 0), (0, 1, 1), (3, 1, 2)]
    + [(1, 0, 2), (3, 0, 1), (1, 0, 1), (3, 0, 2)]
    + [(2, 0, 0), (1, 0, 0), (3, 0, 0), (0, 0, 0)]
    + [(0, 1, 2), (0, 0, 1), (0, 0, 2)]
)
PLACE = {item: q for q, item in enumerate(ORDER)}


def transfer_names():
    names = [("x", 0), ("x", 1)]
    for t in range(2):
        names += [("D", t, j) for j in range(CB)]
        names += [("s1", t, way, dy) for way in range(2) for dy in range(2)]
        names += [("a1", t, dx) for dx in range(4)]
        names += [("in", t, way, dy) for way in range(2) for dy in range(2)]
        names += [("de", t, way, dy) for way in range(2) for dy in range(2)]
        names += [(kind, t, way) for kind in ("fa", "ia", "da") for way in range(2)]
        names += [("b2", t, k) for k in (1, 2)]
    names += [(kind, piece) for kind in ("yo", "r", "l") for piece in PIECES]
    names += [(kind, piece) for kind in ("rp", "lp") for piece in ("2", "1b")]
    names += [("ya", place, piece) for place in "LRF" for piece in ("0", "1a")]
    names += ["rh", "lh0", "lh1"]
    names += [(kind, dy) for kind in ("rf", "lf") for dy in range(2)]
    names += [("d", dx, dy, piece) for dx in range(XN) for dy in range(2) for piece in PIECES]
    return {name: n for n, name in enumerate(names)}


NAMES = transfer_names()


def dot(first, second):
    return jnp.dot(first, second, preferred_element_type=F32)


def low(value):
    return value.astype(BF16)


def total(value):
    return jnp.sum(value, axis=(0, 1), keepdims=True)


def kernel(
    place, owner, listing, feat, act, wts, fac, rts,
    wout, rout,
    xraw, xpeer, xt0, xt1, wbuf, actb, own0, own1, other0, other1, pa, pb, wg, wown, ga, gbuf, fbuf, qbuf,
    fwdb, froml, fromr, ya, fwda, fromla, fromra, yb,
    ssem, rsem, lsem,
):
    xt, db = (xt0, xt1), ((own0, other0), (own1, other1))
    r = lax.axis_index("rep")
    group = lax.axis_index("blk")
    c = lax.rem(r, 2)
    x = lax.rem(r // 2, XN)
    y = r // (2 * XN)

    def rep_of(yy, xx, cc):
        return (yy * XN + xx) * 2 + cc

    def right_by(dx):
        return lax.rem(x + dx, XN)

    def y_of(dy):
        return y if dy == 0 else 1 - y

    def slot(dx, dy, cc, k):
        return OWN * rep_of(y_of(dy), right_by(dx), cc) + k

    sib = rep_of(y, x, 1 - c)
    yp = rep_of(1 - y, x, c)
    xr = rep_of(y, right_by(1), c)
    xl = rep_of(y, right_by(3), c)

    def load(n, src, dst):
        copy = pltpu.make_async_copy(src, dst, lsem.at[n])
        copy.start()
        return copy

    def wait_weights(j):
        columns = wbuf.at[pl.ds(j * RB, RB)]
        pltpu.make_async_copy(columns, columns, lsem.at[j]).wait()

    load_x = [load(CB, feat.at[0], xraw.at[0])]
    load_a = load(CB + 1, act.at[0], actb.at[0])
    for j in range(CB):
        for i in range(RB):
            load(j, wts.at[pl.ds(i * B, B), pl.ds(j * B, B)], wbuf.at[j * RB + i])
    load_x.append(load(CB + 2, feat.at[1], xraw.at[1]))
    load_b = load(CB + 5, act.at[1], actb.at[1])
    load_f = load(CB + 3, fac.at[0], fbuf)
    load_q = load(CB + 4, rts.at[0], qbuf)

    barrier = pltpu.get_barrier_semaphore()
    for partner in (sib, yp, xr, xl):
        pl.semaphore_signal(barrier, inc=1, device_id={"rep": partner}, device_id_type=MESH)
    pl.semaphore_wait(barrier, 4)

    started = []

    def remote(n, src, dst, dev):
        return pltpu.make_async_remote_copy(
            src_ref=src, dst_ref=dst, send_sem=ssem.at[n], recv_sem=rsem.at[n],
            device_id={"rep": dev}, device_id_type=MESH,
        )

    def send(name, src, dst, dev):
        copy = remote(NAMES[name], src, dst, dev)
        copy.start()
        started.append(copy)

    def arrived(name, ref, dev):
        remote(NAMES[name], ref, ref, dev).wait_recv()

    for t in range(2):
        send(("x", t), feat.at[t], xpeer.at[t], sib)

    def turn(src, t, half, i):
        cols = pl.ds(pl.multiple_of(i * B, B), B)
        xt[t][i, :, half * B:(half + 1) * B] = src[t, :, cols].T

    def transpose(src, t, half):
        def one(i, carry):
            turn(src, t, half, i)
            return carry
        lax.fori_loop(0, RB, one, 0)

    def gate(t, ready, block, beside):
        def pair(n, carry):
            columns = (2 * n, 2 * n + 1)
            values = []
            for j in columns:
                ready(j)
            for j in columns:
                value = dot(xraw[t, :, 0:B], block(0, j))
                for i in range(1, RB):
                    value = value + dot(xraw[t, :, i * B:(i + 1) * B], block(i, j))
                values.append(value)
            beside(n)
            for j, value in zip(columns, values):
                sigmoid = 1.0 / (1.0 + jnp.exp(-value))
                slope = sigmoid * (1.0 + value * (1.0 - sigmoid))
                cols = pl.ds(pl.multiple_of(j * B, B), B)
                db[t][0][j] = low(actb[t, :, cols].astype(F32) * slope)
            for j in columns:
                remote(
                    NAMES[("D", t, 0)] + j, db[t][0].at[j], db[t][1].at[j], sib
                ).start()
            return carry
        lax.fori_loop(0, CB // 2, pair, 0)
        for m, (dx, dy, k) in enumerate(ORDER[:2]):
            gbuf[1 + m] = half_product(t, slot(dx, dy, c, k), 0)

    def half_product(t, here, half):
        part = slice(half * B, (half + 1) * B)
        return dot(xt[t][place[0, here], :, part], db[t][half][place[1, here]])

    def wait_dgate(t):
        for j in range(CB):
            own, other = db[t][0].at[j], db[t][1].at[j]
            started.append(remote(NAMES[("D", t, j)], own, other, sib))
            arrived(("D", t, j), other, sib)

    def keep(t, at, value):
        dx, dy, k = ORDER[at]
        value = low(value)
        if k == 0:
            pa[t, 2 * dx + dy, 0:B, :] = value
        elif k == 1:
            pa[t, 2 * dx + dy, B:RA, :] = value[:S]
            pb[t, at, S:B, :] = value[S:]
        else:
            pb[t, at] = value

    def partials(t, first, count):
        for at in range(first, first + count):
            dx, dy, k = ORDER[at]
            here = slot(dx, dy, c, k)
            keep(t, at, half_product(t, here, 0) + half_product(t, here, 1))

    def rows_of(k):
        return pl.ds(S, B - S) if k == 1 else pl.ds(0, B)

    def p(t, dx, dy, k):
        return pb.at[t, PLACE[(dx, dy, k)], rows_of(k)]

    def first(t, dx, dy):
        return pa.at[t, 2 * dx + dy]

    side = ((xr, 1, xl), (xl, 3, xr))
    land = (froml, fromr)
    halves = (pl.ds(0, R0), pl.ds(R0, RA - R0))
    heads = (pl.ds(0, R0), pl.ds(0, RA - R0))
    land_a = (fromla, fromra)

    def reduce_blocks(t, between):
        def start(dy):
            for way in range(2):
                k = 1 + way
                send(("s1", t, way, dy), p(t, 2, dy, k), fwdb.at[t, way, dy, rows_of(k)], side[way][0])

        def near(dy):
            for way in range(2):
                k = 2 - way
                send(
                    ("in", t, way, dy), p(t, side[way][1], dy, k),
                    land[way].at[t, dy, k - 1, rows_of(k)], side[way][0],
                )

        def across(dx):
            send(("a1", t, dx), first(t, dx, 1), ya.at[t, dx], yp)

        def pass_on(dy):
            for way in range(2):
                k = 1 + way
                came = fwdb.at[t, way, dy, rows_of(k)]
                arrived(("s1", t, way, dy), came, side[way][2])
                mine = p(t, side[way][1], dy, k)
                mine[...] = low(mine[...].astype(F32) + came[...].astype(F32))
                send(("de", t, way, dy), mine, land[way].at[t, dy, k - 1, rows_of(k)], side[way][0])

        def add_y(dx):
            arrived(("a1", t, dx), ya.at[t, dx], yp)
            return first(t, dx, 0)[...].astype(F32) + ya[t, dx].astype(F32)

        for m, (dx, dy, k) in enumerate(ORDER[:2]):
            keep(t, m, gbuf[1 + m] + half_product(t, slot(dx, dy, c, k), 1))
        start(1)
        partials(t, 2, 1)
        across(2)
        partials(t, 3, 2)
        start(0)
        partials(t, 5, 2)
        across(1)
        partials(t, 7, 2)
        across(3)
        partials(t, 9, 1)
        near(1)
        partials(t, 10, 2)
        across(0)
        partials(t, 12, 12)
        between()
        pass_on(1)
        first(t, 2, 0)[...] = low(add_y(2))
        for way in range(2):
            send(("fa", t, way), first(t, 2, 0).at[halves[way]], fwda.at[t, way, heads[way]], side[way][0])
        near(0)
        pass_on(0)
        for way in range(2):
            dx = side[way][1]
            first(t, dx, 0)[...] = low(add_y(dx))
            half = halves[1 - way]
            send(("ia", t, way), first(t, dx, 0).at[half], land_a[way].at[t, half], side[way][0])
        ga[...] = add_y(0)
        for k in (2, 1):
            p(t, 0, 1, k)[...] = low(summed(t, 1, k))
            send(("b2", t, k), p(t, 0, 1, k), yb.at[t, k - 1, rows_of(k)], yp)
        for way in range(2):
            came = fwda.at[t, way, heads[way]]
            arrived(("fa", t, way), came, side[way][2])
            mine = first(t, side[way][1], 0).at[halves[way]]
            mine[...] = low(mine[...].astype(F32) + came[...].astype(F32))
            send(("da", t, way), mine, land_a[way].at[t, halves[way]], side[way][0])

    def summed(t, dy, k):
        value = p(t, 0, dy, k)[...].astype(F32)
        for way in range(2):
            kind = "de" if k == 1 + way else "in"
            came = land[way].at[t, dy, k - 1, rows_of(k)]
            arrived((kind, t, way, dy), came, side[way][2])
            value = value + came[...].astype(F32)
        return value

    def finish_second(t, k):
        value = summed(t, 0, k)
        came = yb.at[t, k - 1, rows_of(k)]
        arrived(("b2", t, k), came, yp)
        gbuf[k, S if k == 1 else 0:B, :] = value + came[...].astype(F32)

    def finish_first(t):
        for way in range(2):
            for kind, half in (("ia", halves[1 - way]), ("da", halves[way])):
                arrived((kind, t, way), land_a[way].at[t, half], side[way][2])
        value = ga[...] + fromla[t].astype(F32) + fromra[t].astype(F32)
        gbuf[0] = value[:B]
        gbuf[1, 0:S, :] = value[B:]

    def update(ks):
        grads = [gbuf[k] for k in ks]
        lefts = [low(dot(qbuf[k, 0], low(grad))) for k, grad in zip(ks, grads)]
        shaped = [dot(left, qbuf[k, 1]) for k, left in zip(ks, lefts)]
        grad_norms = [jnp.sqrt(total(grad * grad) + NORM_EPS) for grad in grads]
        shaped_norms = [jnp.sqrt(total(value * value) + NORM_EPS) for value in shaped]
        for k, value, top, bottom in zip(ks, shaped, grad_norms, shaped_norms):
            wown[k] = low(wown[k].astype(F32) - STEP_SIZE * (top / bottom) * value)

    def refresh(t, owned):
        rows = lax.broadcasted_iota(jnp.int32, (B, B), 0)
        cols = lax.broadcasted_iota(jnp.int32, (B, B), 1)
        diagonal = rows == cols
        five = jnp.where(diagonal, F32(5.0), F32(0.0))
        ridge = jnp.where(diagonal, F32(RIDGE), F32(0.0))
        sides = [(k, e) for k in owned for e in range(2)]
        stats = []
        for k in owned:
            grad = low(gbuf[k])
            turned = grad.T
            stats += [dot(grad, turned), dot(turned, grad)]
        current, factor, result = [], [], []
        for (k, e), stat in zip(sides, stats):
            fresh = DECAY * fbuf[k, e] + (1.0 - DECAY) * stat
            fbuf[k, e] = fresh
            ridged = fresh + ridge
            scale = jnp.sqrt(total(ridged * ridged) + NORM_EPS)
            current.append(ridged / scale)
            factor.append((five - current[-1]) * 0.25)
            result.append(low(factor[-1] / jnp.sqrt(jnp.sqrt(scale))))
        for turn in range(1, NEWTON):
            factor = [low(value) for value in factor]
            square = [low(dot(value, value)) for value in factor]
            fourth = [low(dot(value, value)) for value in square]
            current = [dot(value, low(old)) for value, old in zip(fourth, current)]
            factor = [(five - value) * 0.25 for value in current]
            result = [low(dot(old, low(value))) for old, value in zip(result, factor)]
        for (k, e), value in zip(sides, result):
            name = group * (2 * OWN) + 2 * k + e
            hits = total(jnp.where(listing[t] == name, F32(1.0), F32(0.0)))
            qbuf[k, e] = jnp.where(hits > 0.5, value, qbuf[k, e])

    def w_at(dx, dy, piece):
        k, begin, rows = PIECES[piece]
        return wg.at[slot(dx, dy, c, k), pl.ds(begin, rows)]

    def share(dx, dy, piece):
        ref = w_at(dx, dy, piece)
        send(("d", dx, dy, piece), ref, ref, sib)

    def gather_blocks():
        def ship(name, ref, dev):
            send(name, ref, ref, dev)

        def spread(piece):
            ref = w_at(0, 0, piece)
            ship(("yo", piece), ref, yp)
            ship(("r", piece), ref, xr)
            ship(("l", piece), ref, xl)
            share(0, 0, piece)

        def renew(ks):
            update(ks)
            for k in ks:
                wg[slot(0, 0, c, k)] = wown[k]

        def expect(name, dx, dy, piece, dev):
            arrived(name, w_at(dx, dy, piece), dev)
            share(dx, dy, piece)

        finish_second(0, 2)
        renew((2,))
        spread("2")
        finish_second(0, 1)
        finish_first(0)
        renew((1, 0))
        spread("1b")
        spread("0")
        spread("1a")
        refresh(0, (2,))
        expect(("r", "2"), 3, 0, "2", xl)
        expect(("l", "2"), 1, 0, "2", xr)
        refresh(0, (1,))
        for piece in ("2", "1b"):
            expect(("yo", piece), 0, 1, piece, yp)
            ship(("rp", piece), w_at(0, 1, piece), xr)
            ship(("lp", piece), w_at(0, 1, piece), xl)
        expect(("r", "1b"), 3, 0, "1b", xl)
        expect(("l", "1b"), 1, 0, "1b", xr)
        top, bottom = pl.ds(0, R0), pl.ds(R0, B - R0)
        expect(("r", "0"), 3, 0, "0", xl)
        ship("rh", wg.at[slot(3, 0, c, 0), top], xr)
        expect(("l", "0"), 1, 0, "0", xr)
        ship("lh0", wg.at[slot(1, 0, c, 0), bottom], xl)
        ship(("ya", "L", "0"), w_at(3, 0, "0"), yp)
        ship(("ya", "R", "0"), w_at(1, 0, "0"), yp)
        expect(("r", "1a"), 3, 0, "1a", xl)
        expect(("l", "1a"), 1, 0, "1a", xr)
        ship("lh1", w_at(1, 0, "1a"), xl)
        ship(("ya", "L", "1a"), w_at(3, 0, "1a"), yp)
        ship(("ya", "R", "1a"), w_at(1, 0, "1a"), yp)
        ship(("rf", 0), w_at(3, 0, "1b"), xr)
        ship(("lf", 0), w_at(1, 0, "2"), xl)
        refresh(0, (0,))
        for piece in ("0", "1a"):
            expect(("yo", piece), 0, 1, piece, yp)
        for piece in ("2", "1b"):
            expect(("rp", piece), 3, 1, piece, xl)
            if piece == "1b":
                ship(("rf", 1), w_at(3, 1, piece), xr)
            expect(("lp", piece), 1, 1, piece, xr)
            if piece == "2":
                ship(("lf", 1), w_at(1, 1, piece), xl)
        expect(("ya", "L", "0"), 3, 1, "0", yp)
        arrived("rh", wg.at[slot(2, 0, c, 0), top], xl)
        arrived("lh0", wg.at[slot(2, 0, c, 0), bottom], xr)
        ship(("ya", "F", "0"), w_at(2, 0, "0"), yp)
        share(2, 0, "0")
        expect("lh1", 2, 0, "1a", xr)
        ship(("ya", "F", "1a"), w_at(2, 0, "1a"), yp)
        expect(("ya", "R", "0"), 1, 1, "0", yp)
        expect(("ya", "L", "1a"), 3, 1, "1a", yp)
        expect(("ya", "R", "1a"), 1, 1, "1a", yp)
        for dy in range(2):
            expect(("rf", dy), 2, dy, "1b", xl)
            expect(("lf", dy), 2, dy, "2", xr)
        for piece in ("0", "1a"):
            expect(("ya", "F", piece), 2, 1, piece, yp)
        for dx in range(XN):
            for dy in range(2):
                for piece, (k, begin, rows) in PIECES.items():
                    ref = wg.at[slot(dx, dy, 1 - c, k), pl.ds(begin, rows)]
                    arrived(("d", dx, dy, piece), ref, sib)

    load_x[0].wait()
    load_a.wait()

    def turn_own(n):
        for m in range(3):
            turn(xraw, 0, 0, jnp.minimum(3 * n + m, RB - 1))

    gate(0, wait_weights, lambda i, j: wbuf[j * RB + i], turn_own)
    arrived(("x", 0), xpeer.at[0], sib)
    transpose(xpeer, 0, 1)
    wait_dgate(0)

    def meanwhile():
        for k in range(OWN):
            wown[k] = wbuf[place[2, OWN * r + k]]
        load_x[1].wait()
        transpose(xraw, 1, 0)
        arrived(("x", 1), xpeer.at[1], sib)
        transpose(xpeer, 1, 1)
        load_b.wait()
        load_f.wait()
        load_q.wait()

    reduce_blocks(0, meanwhile)
    gather_blocks()

    gate(1, lambda j: None, lambda i, j: wg[owner[0, i * CB + j]], lambda n: None)
    wait_dgate(1)
    reduce_blocks(1, lambda: None)
    results = []

    def conclude(ks):
        def put(src, dst):
            results.append(load(CB + 6 + len(results), src, dst))

        update(ks)
        for k in ks:
            put(wown.at[k], wout.at[0, k])
        refresh(1, ks)
        for k in ks:
            put(qbuf.at[k], rout.at[0, k])

    finish_second(1, 2)
    conclude((2,))
    finish_second(1, 1)
    finish_first(1)
    conclude((1, 0))
    for copy in results:
        copy.wait()
    for copy in started:
        copy.wait_send()


def deliver(weights, roots, wout, rout, held, insem, outsem):
    pieces = [(weights.at[0, k], wout.at[0, k]) for k in range(OWN)]
    pieces += [(roots.at[0, k, e], rout.at[0, k, e]) for k in range(OWN) for e in range(2)]
    incoming, outgoing = [], []
    for n, (src, dst) in enumerate(pieces):
        incoming.append(pltpu.make_async_copy(src, held.at[n], insem.at[n]))
        outgoing.append(pltpu.make_async_copy(held.at[n], dst, outsem.at[n]))
        incoming[n].start()
    for n in range(len(pieces)):
        incoming[n].wait()
        outgoing[n].start()
    for n in range(len(pieces)):
        outgoing[n].wait()


def body(features, grad_act, weights, owner_slot, factors, roots, helper_list):
    ids = jnp.arange(RB * CB, dtype=jnp.int32)
    rows, cols = ids // CB, ids % CB
    kinds = jnp.arange(3, dtype=jnp.int32)[:, None]
    wanted = jnp.where(kinds == 0, rows, jnp.where(kinds == 1, cols, cols * RB + rows))
    placing = owner_slot[0][None, :] == ids[:, None]
    place = jnp.sum(jnp.where(placing[None], wanted[:, None, :], 0), axis=2)
    listing = jnp.swapaxes(helper_list, 1, 2)
    tokens = features.shape[1]
    anywhere = pl.BlockSpec(memory_space=pl.ANY)
    scalars = pl.BlockSpec(memory_space=pltpu.SMEM)
    local = pl.BlockSpec(memory_space=pltpu.VMEM)
    block = (B, B)
    results = (
        jax.ShapeDtypeStruct((1, OWN) + block, BF16),
        jax.ShapeDtypeStruct((1, OWN, 2) + block, BF16),
    )
    made = pl.pallas_call(
        kernel,
        out_shape=results,
        in_specs=[scalars, scalars, local] + [anywhere] * 5,
        out_specs=(anywhere, anywhere),
        scratch_shapes=[
            pltpu.VMEM((2, tokens, RB * B), BF16),
            pltpu.VMEM((2, tokens, RB * B), BF16),
            pltpu.VMEM((RB, B, 2 * tokens), BF16),
            pltpu.VMEM((RB, B, 2 * tokens), BF16),
            pltpu.VMEM((CB * RB,) + block, BF16),
            pltpu.VMEM((2, tokens, CB * B), BF16),
            pltpu.VMEM((CB, tokens, B), BF16),
            pltpu.VMEM((CB, tokens, B), BF16),
            pltpu.VMEM((CB, tokens, B), BF16),
            pltpu.VMEM((CB, tokens, B), BF16),
            pltpu.VMEM((2, 2 * XN, RA, B), BF16),
            pltpu.VMEM((2, len(ORDER)) + block, BF16),
            pltpu.VMEM((RB * CB,) + block, BF16),
            pltpu.VMEM((OWN,) + block, BF16),
            pltpu.VMEM((RA, B), F32),
            pltpu.VMEM((OWN,) + block, F32),
            pltpu.VMEM((OWN, 2) + block, F32),
            pltpu.VMEM((OWN, 2) + block, BF16),
            pltpu.VMEM((2, 2, 2) + block, BF16),
            pltpu.VMEM((2, 2, 2) + block, BF16),
            pltpu.VMEM((2, 2, 2) + block, BF16),
            pltpu.VMEM((2, XN, RA, B), BF16),
            pltpu.VMEM((2, 2, R0, B), BF16),
            pltpu.VMEM((2, RA, B), BF16),
            pltpu.VMEM((2, RA, B), BF16),
            pltpu.VMEM((2, 2) + block, BF16),
            pltpu.SemaphoreType.DMA((len(NAMES),)),
            pltpu.SemaphoreType.DMA((len(NAMES),)),
            pltpu.SemaphoreType.DMA((CB + 6 + 2 * OWN,)),
        ],
        compiler_params=pltpu.CompilerParams(
            collective_id=0, has_side_effects=True, vmem_limit_bytes=60 * 1024 * 1024
        ),
    )(place, owner_slot, listing, features, grad_act, weights, factors, roots)
    return pl.pallas_call(
        deliver,
        out_shape=results,
        in_specs=[anywhere] * 2,
        out_specs=(anywhere, anywhere),
        scratch_shapes=[
            pltpu.VMEM((3 * OWN,) + block, BF16),
            pltpu.SemaphoreType.DMA((3 * OWN,)),
            pltpu.SemaphoreType.DMA((3 * OWN,)),
        ],
    )(*made)


def solution(mesh):
    return jax.shard_map(
        body,
        mesh=mesh,
        in_specs=(
            P(None, "rep", None),
            P(None, "rep", "blk"),
            P(None, "blk"),
            P("blk", None),
            P("blk", "rep", None, None, None),
            P("blk", "rep", None, None, None),
            P(),
        ),
        out_specs=(P("blk", "rep", None, None), P("blk", "rep", None, None, None)),
        check_vma=False,
    )
```

```python
import jax
import jax.numpy as jnp
from jax import lax
from jax.experimental import pallas as pl
from jax.experimental.pallas import tpu as pltpu
from jax.sharding import PartitionSpec as P

NEWTON = 3
RIDGE = 0.001
NORM_EPS = 1e-06
DECAY = 0.95
STEP_SIZE = 0.5

B = 256
S = 80
RA = B + S
R0 = 240
PIECES = {"0": (0, 0, B), "1a": (1, 0, S), "1b": (1, S, B - S), "2": (2, 0, B)}
OWN = 3
RB = 8
CB = 6
XN = 4
F32 = jnp.float32
BF16 = jnp.bfloat16
MESH = pl.DeviceIdType.MESH

ORDER = (
    [(2, 1, 1), (2, 1, 2), (2, 1, 0), (2, 0, 1), (2, 0, 2)]
    + [(1, 1, 0), (1, 1, 1), (3, 1, 0), (3, 1, 1), (1, 1, 2)]
    + [(0, 1, 0), (0, 1, 1), (3, 1, 2)]
    + [(1, 0, 2), (3, 0, 1), (1, 0, 1), (3, 0, 2)]
    + [(2, 0, 0), (1, 0, 0), (3, 0, 0), (0, 0, 0)]
    + [(0, 1, 2), (0, 0, 1), (0, 0, 2)]
)
PLACE = {item: q for q, item in enumerate(ORDER)}


def transfer_names():
    names = [("x", 0), ("x", 1)]
    for t in range(2):
        names += [("D", t, j) for j in range(CB)]
        names += [("s1", t, way, dy) for way in range(2) for dy in range(2)]
        names += [("a1", t, dx) for dx in range(4)]
        names += [("in", t, way, dy) for way in range(2) for dy in range(2)]
        names += [("de", t, way, dy) for way in range(2) for dy in range(2)]
        names += [(kind, t, way) for kind in ("fa", "ia", "da") for way in range(2)]
        names += [("b2", t, k) for k in (1, 2)]
    names += [(kind, piece) for kind in ("yo", "r", "l") for piece in PIECES]
    names += [(kind, piece) for kind in ("rp", "lp") for piece in ("2", "1b")]
    names += [("ya", place, piece) for place in "LRF" for piece in ("0", "1a")]
    names += ["rh", "lh0", "lh1"]
    names += [(kind, dy) for kind in ("rf", "lf") for dy in range(2)]
    names += [("d", dx, dy, piece) for dx in range(XN) for dy in range(2) for piece in PIECES]
    return {name: n for n, name in enumerate(names)}


NAMES = transfer_names()


def dot(first, second):
    return jnp.dot(first, second, preferred_element_type=F32)


def low(value):
    return value.astype(BF16)


def total(value):
    return jnp.sum(value, axis=(0, 1), keepdims=True)


def kernel(
    place, owner, listing, feat, act, wts, fac, rts,
    wout, rout,
    xraw, xpeer, xt0, xt1, wbuf, actb, own0, own1, other0, other1, pa, pb, wg, wown, ga, gbuf, fbuf, qbuf,
    fwdb, froml, fromr, ya, fwda, fromla, fromra, yb,
    ssem, rsem, lsem,
):
    xt, db = (xt0, xt1), ((own0, other0), (own1, other1))
    r = lax.axis_index("rep")
    group = lax.axis_index("blk")
    c = lax.rem(r, 2)
    x = lax.rem(r // 2, XN)
    y = r // (2 * XN)

    def rep_of(yy, xx, cc):
        return (yy * XN + xx) * 2 + cc

    def right_by(dx):
        return lax.rem(x + dx, XN)

    def y_of(dy):
        return y if dy == 0 else 1 - y

    def slot(dx, dy, cc, k):
        return OWN * rep_of(y_of(dy), right_by(dx), cc) + k

    sib = rep_of(y, x, 1 - c)
    yp = rep_of(1 - y, x, c)
    xr = rep_of(y, right_by(1), c)
    xl = rep_of(y, right_by(3), c)

    def load(n, src, dst):
        copy = pltpu.make_async_copy(src, dst, lsem.at[n])
        copy.start()
        return copy

    def wait_weights(j):
        columns = wbuf.at[pl.ds(j * RB, RB)]
        pltpu.make_async_copy(columns, columns, lsem.at[j]).wait()

    load_x = [load(CB, feat.at[0], xraw.at[0])]
    load_a = load(CB + 1, act.at[0], actb.at[0])
    for j in range(CB):
        for i in range(RB):
            load(j, wts.at[pl.ds(i * B, B), pl.ds(j * B, B)], wbuf.at[j * RB + i])
    load_x.append(load(CB + 2, feat.at[1], xraw.at[1]))
    load_b = load(CB + 5, act.at[1], actb.at[1])
    load_f = load(CB + 3, fac.at[0], fbuf)
    load_q = load(CB + 4, rts.at[0], qbuf)

    barrier = pltpu.get_barrier_semaphore()
    for partner in (sib, yp, xr, xl):
        pl.semaphore_signal(barrier, inc=1, device_id={"rep": partner}, device_id_type=MESH)
    pl.semaphore_wait(barrier, 4)

    started = []

    def remote(n, src, dst, dev):
        return pltpu.make_async_remote_copy(
            src_ref=src, dst_ref=dst, send_sem=ssem.at[n], recv_sem=rsem.at[n],
            device_id={"rep": dev}, device_id_type=MESH,
        )

    def send(name, src, dst, dev):
        copy = remote(NAMES[name], src, dst, dev)
        copy.start()
        started.append(copy)

    def arrived(name, ref, dev):
        remote(NAMES[name], ref, ref, dev).wait_recv()

    for t in range(2):
        send(("x", t), feat.at[t], xpeer.at[t], sib)

    def turn(src, t, half, i):
        cols = pl.ds(pl.multiple_of(i * B, B), B)
        xt[t][i, :, half * B:(half + 1) * B] = src[t, :, cols].T

    def transpose(src, t, half):
        def one(i, carry):
            turn(src, t, half, i)
            return carry
        lax.fori_loop(0, RB, one, 0)

    def gate(t, ready, block, beside):
        def pair(n, carry):
            columns = (2 * n, 2 * n + 1)
            values = []
            for j in columns:
                ready(j)
            for j in columns:
                value = dot(xraw[t, :, 0:B], block(0, j))
                for i in range(1, RB):
                    value = value + dot(xraw[t, :, i * B:(i + 1) * B], block(i, j))
                values.append(value)
            beside(n)
            for j, value in zip(columns, values):
                sigmoid = 1.0 / (1.0 + jnp.exp(-value))
                slope = sigmoid * (1.0 + value * (1.0 - sigmoid))
                cols = pl.ds(pl.multiple_of(j * B, B), B)
                db[t][0][j] = low(actb[t, :, cols].astype(F32) * slope)
            for j in columns:
                remote(
                    NAMES[("D", t, 0)] + j, db[t][0].at[j], db[t][1].at[j], sib
                ).start()
            return carry
        lax.fori_loop(0, CB // 2, pair, 0)
        for m, (dx, dy, k) in enumerate(ORDER[:2]):
            gbuf[1 + m] = half_product(t, slot(dx, dy, c, k), 0)

    def half_product(t, here, half):
        part = slice(half * B, (half + 1) * B)
        return dot(xt[t][place[0, here], :, part], db[t][half][place[1, here]])

    def wait_dgate(t):
        for j in range(CB):
            own, other = db[t][0].at[j], db[t][1].at[j]
            started.append(remote(NAMES[("D", t, j)], own, other, sib))
            arrived(("D", t, j), other, sib)

    def keep(t, at, value):
        dx, dy, k = ORDER[at]
        value = low(value)
        if k == 0:
            pa[t, 2 * dx + dy, 0:B, :] = value
        elif k == 1:
            pa[t, 2 * dx + dy, B:RA, :] = value[:S]
            pb[t, at, S:B, :] = value[S:]
        else:
            pb[t, at] = value

    def partials(t, first, count):
        for at in range(first, first + count):
            dx, dy, k = ORDER[at]
            here = slot(dx, dy, c, k)
            keep(t, at, half_product(t, here, 0) + half_product(t, here, 1))

    def rows_of(k):
        return pl.ds(S, B - S) if k == 1 else pl.ds(0, B)

    def p(t, dx, dy, k):
        return pb.at[t, PLACE[(dx, dy, k)], rows_of(k)]

    def first(t, dx, dy):
        return pa.at[t, 2 * dx + dy]

    side = ((xr, 1, xl), (xl, 3, xr))
    land = (froml, fromr)
    halves = (pl.ds(0, R0), pl.ds(R0, RA - R0))
    heads = (pl.ds(0, R0), pl.ds(0, RA - R0))
    land_a = (fromla, fromra)

    def reduce_blocks(t, between):
        def start(dy):
            for way in range(2):
                k = 1 + way
                send(("s1", t, way, dy), p(t, 2, dy, k), fwdb.at[t, way, dy, rows_of(k)], side[way][0])

        def near(dy):
            for way in range(2):
                k = 2 - way
                send(
                    ("in", t, way, dy), p(t, side[way][1], dy, k),
                    land[way].at[t, dy, k - 1, rows_of(k)], side[way][0],
                )

        def across(dx):
            send(("a1", t, dx), first(t, dx, 1), ya.at[t, dx], yp)

        def pass_on(dy):
            for way in range(2):
                k = 1 + way
                came = fwdb.at[t, way, dy, rows_of(k)]
                arrived(("s1", t, way, dy), came, side[way][2])
                mine = p(t, side[way][1], dy, k)
                mine[...] = low(mine[...].astype(F32) + came[...].astype(F32))
                send(("de", t, way, dy), mine, land[way].at[t, dy, k - 1, rows_of(k)], side[way][0])

        def add_y(dx):
            arrived(("a1", t, dx), ya.at[t, dx], yp)
            return first(t, dx, 0)[...].astype(F32) + ya[t, dx].astype(F32)

        for m, (dx, dy, k) in enumerate(ORDER[:2]):
            keep(t, m, gbuf[1 + m] + half_product(t, slot(dx, dy, c, k), 1))
        start(1)
        partials(t, 2, 1)
        across(2)
        partials(t, 3, 2)
        start(0)
        partials(t, 5, 2)
        across(1)
        partials(t, 7, 2)
        across(3)
        partials(t, 9, 1)
        near(1)
        partials(t, 10, 2)
        across(0)
        partials(t, 12, 12)
        pass_on(1)
        between()
        first(t, 2, 0)[...] = low(add_y(2))
        for way in range(2):
            send(("fa", t, way), first(t, 2, 0).at[halves[way]], fwda.at[t, way, heads[way]], side[way][0])
        near(0)
        pass_on(0)
        for way in range(2):
            dx = side[way][1]
            first(t, dx, 0)[...] = low(add_y(dx))
            half = halves[1 - way]
            send(("ia", t, way), first(t, dx, 0).at[half], land_a[way].at[t, half], side[way][0])
        ga[...] = add_y(0)
        for k in (2, 1):
            p(t, 0, 1, k)[...] = low(summed(t, 1, k))
            send(("b2", t, k), p(t, 0, 1, k), yb.at[t, k - 1, rows_of(k)], yp)
        for way in range(2):
            came = fwda.at[t, way, heads[way]]
            arrived(("fa", t, way), came, side[way][2])
            mine = first(t, side[way][1], 0).at[halves[way]]
            mine[...] = low(mine[...].astype(F32) + came[...].astype(F32))
            send(("da", t, way), mine, land_a[way].at[t, halves[way]], side[way][0])

    def summed(t, dy, k):
        value = p(t, 0, dy, k)[...].astype(F32)
        for way in range(2):
            kind = "de" if k == 1 + way else "in"
            came = land[way].at[t, dy, k - 1, rows_of(k)]
            arrived((kind, t, way, dy), came, side[way][2])
            value = value + came[...].astype(F32)
        return value

    def finish_second(t, k):
        value = summed(t, 0, k)
        came = yb.at[t, k - 1, rows_of(k)]
        arrived(("b2", t, k), came, yp)
        gbuf[k, S if k == 1 else 0:B, :] = value + came[...].astype(F32)

    def finish_first(t):
        for way in range(2):
            for kind, half in (("ia", halves[1 - way]), ("da", halves[way])):
                arrived((kind, t, way), land_a[way].at[t, half], side[way][2])
        value = ga[...] + fromla[t].astype(F32) + fromra[t].astype(F32)
        gbuf[0] = value[:B]
        gbuf[1, 0:S, :] = value[B:]

    def update(ks):
        grads = [gbuf[k] for k in ks]
        lefts = [low(dot(qbuf[k, 0], low(grad))) for k, grad in zip(ks, grads)]
        shaped = [dot(left, qbuf[k, 1]) for k, left in zip(ks, lefts)]
        grad_norms = [jnp.sqrt(total(grad * grad) + NORM_EPS) for grad in grads]
        shaped_norms = [jnp.sqrt(total(value * value) + NORM_EPS) for value in shaped]
        for k, value, top, bottom in zip(ks, shaped, grad_norms, shaped_norms):
            wown[k] = low(wown[k].astype(F32) - STEP_SIZE * (top / bottom) * value)

    def refresh(t, owned):
        rows = lax.broadcasted_iota(jnp.int32, (B, B), 0)
        cols = lax.broadcasted_iota(jnp.int32, (B, B), 1)
        diagonal = rows == cols
        five = jnp.where(diagonal, F32(5.0), F32(0.0))
        ridge = jnp.where(diagonal, F32(RIDGE), F32(0.0))
        sides = [(k, e) for k in owned for e in range(2)]
        stats = []
        for k in owned:
            grad = low(gbuf[k])
            turned = grad.T
            stats += [dot(grad, turned), dot(turned, grad)]
        current, factor, result = [], [], []
        for (k, e), stat in zip(sides, stats):
            fresh = DECAY * fbuf[k, e] + (1.0 - DECAY) * stat
            fbuf[k, e] = fresh
            ridged = fresh + ridge
            scale = jnp.sqrt(total(ridged * ridged) + NORM_EPS)
            current.append(ridged / scale)
            factor.append((five - current[-1]) * 0.25)
            result.append(low(factor[-1] / jnp.sqrt(jnp.sqrt(scale))))
        for turn in range(1, NEWTON):
            factor = [low(value) for value in factor]
            square = [low(dot(value, value)) for value in factor]
            fourth = [low(dot(value, value)) for value in square]
            current = [dot(value, low(old)) for value, old in zip(fourth, current)]
            factor = [(five - value) * 0.25 for value in current]
            result = [low(dot(old, low(value))) for old, value in zip(result, factor)]
        for (k, e), value in zip(sides, result):
            name = group * (2 * OWN) + 2 * k + e
            hits = total(jnp.where(listing[t] == name, F32(1.0), F32(0.0)))
            qbuf[k, e] = jnp.where(hits > 0.5, value, qbuf[k, e])

    def w_at(dx, dy, piece):
        k, begin, rows = PIECES[piece]
        return wg.at[slot(dx, dy, c, k), pl.ds(begin, rows)]

    def share(dx, dy, piece):
        ref = w_at(dx, dy, piece)
        send(("d", dx, dy, piece), ref, ref, sib)

    def gather_blocks():
        def ship(name, ref, dev):
            send(name, ref, ref, dev)

        def spread(piece):
            ref = w_at(0, 0, piece)
            ship(("yo", piece), ref, yp)
            ship(("r", piece), ref, xr)
            ship(("l", piece), ref, xl)
            share(0, 0, piece)

        def renew(ks):
            update(ks)
            for k in ks:
                wg[slot(0, 0, c, k)] = wown[k]

        def expect(name, dx, dy, piece, dev):
            arrived(name, w_at(dx, dy, piece), dev)
            share(dx, dy, piece)

        finish_second(0, 2)
        renew((2,))
        spread("2")
        finish_second(0, 1)
        finish_first(0)
        renew((1, 0))
        spread("1b")
        spread("0")
        spread("1a")
        refresh(0, (2,))
        expect(("r", "2"), 3, 0, "2", xl)
        expect(("l", "2"), 1, 0, "2", xr)
        refresh(0, (1,))
        for piece in ("2", "1b"):
            expect(("yo", piece), 0, 1, piece, yp)
            ship(("rp", piece), w_at(0, 1, piece), xr)
            ship(("lp", piece), w_at(0, 1, piece), xl)
        expect(("r", "1b"), 3, 0, "1b", xl)
        expect(("l", "1b"), 1, 0, "1b", xr)
        top, bottom = pl.ds(0, R0), pl.ds(R0, B - R0)
        expect(("r", "0"), 3, 0, "0", xl)
        ship("rh", wg.at[slot(3, 0, c, 0), top], xr)
        expect(("l", "0"), 1, 0, "0", xr)
        ship("lh0", wg.at[slot(1, 0, c, 0), bottom], xl)
        ship(("ya", "L", "0"), w_at(3, 0, "0"), yp)
        ship(("ya", "R", "0"), w_at(1, 0, "0"), yp)
        expect(("r", "1a"), 3, 0, "1a", xl)
        expect(("l", "1a"), 1, 0, "1a", xr)
        ship("lh1", w_at(1, 0, "1a"), xl)
        ship(("ya", "L", "1a"), w_at(3, 0, "1a"), yp)
        ship(("ya", "R", "1a"), w_at(1, 0, "1a"), yp)
        ship(("rf", 0), w_at(3, 0, "1b"), xr)
        ship(("lf", 0), w_at(1, 0, "2"), xl)
        refresh(0, (0,))
        for piece in ("0", "1a"):
            expect(("yo", piece), 0, 1, piece, yp)
        for piece in ("2", "1b"):
            expect(("rp", piece), 3, 1, piece, xl)
            if piece == "1b":
                ship(("rf", 1), w_at(3, 1, piece), xr)
            expect(("lp", piece), 1, 1, piece, xr)
            if piece == "2":
                ship(("lf", 1), w_at(1, 1, piece), xl)
        expect(("ya", "L", "0"), 3, 1, "0", yp)
        arrived("rh", wg.at[slot(2, 0, c, 0), top], xl)
        arrived("lh0", wg.at[slot(2, 0, c, 0), bottom], xr)
        ship(("ya", "F", "0"), w_at(2, 0, "0"), yp)
        share(2, 0, "0")
        expect("lh1", 2, 0, "1a", xr)
        ship(("ya", "F", "1a"), w_at(2, 0, "1a"), yp)
        expect(("ya", "R", "0"), 1, 1, "0", yp)
        expect(("ya", "L", "1a"), 3, 1, "1a", yp)
        expect(("ya", "R", "1a"), 1, 1, "1a", yp)
        for dy in range(2):
            expect(("rf", dy), 2, dy, "1b", xl)
            expect(("lf", dy), 2, dy, "2", xr)
        for piece in ("0", "1a"):
            expect(("ya", "F", piece), 2, 1, piece, yp)
        for dx in range(XN):
            for dy in range(2):
                for piece, (k, begin, rows) in PIECES.items():
                    ref = wg.at[slot(dx, dy, 1 - c, k), pl.ds(begin, rows)]
                    arrived(("d", dx, dy, piece), ref, sib)

    load_x[0].wait()
    load_a.wait()

    def turn_own(n):
        for m in range(3):
            turn(xraw, 0, 0, jnp.minimum(3 * n + m, RB - 1))

    gate(0, wait_weights, lambda i, j: wbuf[j * RB + i], turn_own)
    arrived(("x", 0), xpeer.at[0], sib)
    transpose(xpeer, 0, 1)
    wait_dgate(0)

    def meanwhile():
        for k in range(OWN):
            wown[k] = wbuf[place[2, OWN * r + k]]
        load_x[1].wait()
        transpose(xraw, 1, 0)
        arrived(("x", 1), xpeer.at[1], sib)
        transpose(xpeer, 1, 1)
        load_b.wait()
        load_f.wait()
        load_q.wait()

    reduce_blocks(0, meanwhile)
    gather_blocks()

    gate(1, lambda j: None, lambda i, j: wg[owner[0, i * CB + j]], lambda n: None)
    wait_dgate(1)
    reduce_blocks(1, lambda: None)
    results = []

    def conclude(ks):
        def put(src, dst):
            results.append(load(CB + 6 + len(results), src, dst))

        update(ks)
        for k in ks:
            put(wown.at[k], wout.at[0, k])
        refresh(1, ks)
        for k in ks:
            put(qbuf.at[k], rout.at[0, k])

    finish_second(1, 2)
    conclude((2,))
    finish_second(1, 1)
    finish_first(1)
    conclude((1, 0))
    for copy in results:
        copy.wait()
    for copy in started:
        copy.wait_send()


def deliver(weights, roots, wout, rout, held, insem, outsem):
    pieces = [(weights.at[0, k], wout.at[0, k]) for k in range(OWN)]
    pieces += [(roots.at[0, k, e], rout.at[0, k, e]) for k in range(OWN) for e in range(2)]
    incoming, outgoing = [], []
    for n, (src, dst) in enumerate(pieces):
        incoming.append(pltpu.make_async_copy(src, held.at[n], insem.at[n]))
        outgoing.append(pltpu.make_async_copy(held.at[n], dst, outsem.at[n]))
        incoming[n].start()
    for n in range(len(pieces)):
        incoming[n].wait()
        outgoing[n].start()
    for n in range(len(pieces)):
        outgoing[n].wait()


def body(features, grad_act, weights, owner_slot, factors, roots, helper_list):
    ids = jnp.arange(RB * CB, dtype=jnp.int32)
    rows, cols = ids // CB, ids % CB
    kinds = jnp.arange(3, dtype=jnp.int32)[:, None]
    wanted = jnp.where(kinds == 0, rows, jnp.where(kinds == 1, cols, cols * RB + rows))
    placing = owner_slot[0][None, :] == ids[:, None]
    place = jnp.sum(jnp.where(placing[None], wanted[:, None, :], 0), axis=2)
    listing = jnp.swapaxes(helper_list, 1, 2)
    tokens = features.shape[1]
    anywhere = pl.BlockSpec(memory_space=pl.ANY)
    scalars = pl.BlockSpec(memory_space=pltpu.SMEM)
    local = pl.BlockSpec(memory_space=pltpu.VMEM)
    block = (B, B)
    results = (
        jax.ShapeDtypeStruct((1, OWN) + block, BF16),
        jax.ShapeDtypeStruct((1, OWN, 2) + block, BF16),
    )
    made = pl.pallas_call(
        kernel,
        out_shape=results,
        in_specs=[scalars, scalars, local] + [anywhere] * 5,
        out_specs=(anywhere, anywhere),
        scratch_shapes=[
            pltpu.VMEM((2, tokens, RB * B), BF16),
            pltpu.VMEM((2, tokens, RB * B), BF16),
            pltpu.VMEM((RB, B, 2 * tokens), BF16),
            pltpu.VMEM((RB, B, 2 * tokens), BF16),
            pltpu.VMEM((CB * RB,) + block, BF16),
            pltpu.VMEM((2, tokens, CB * B), BF16),
            pltpu.VMEM((CB, tokens, B), BF16),
            pltpu.VMEM((CB, tokens, B), BF16),
            pltpu.VMEM((CB, tokens, B), BF16),
            pltpu.VMEM((CB, tokens, B), BF16),
            pltpu.VMEM((2, 2 * XN, RA, B), BF16),
            pltpu.VMEM((2, len(ORDER)) + block, BF16),
            pltpu.VMEM((RB * CB,) + block, BF16),
            pltpu.VMEM((OWN,) + block, BF16),
            pltpu.VMEM((RA, B), F32),
            pltpu.VMEM((OWN,) + block, F32),
            pltpu.VMEM((OWN, 2) + block, F32),
            pltpu.VMEM((OWN, 2) + block, BF16),
            pltpu.VMEM((2, 2, 2) + block, BF16),
            pltpu.VMEM((2, 2, 2) + block, BF16),
            pltpu.VMEM((2, 2, 2) + block, BF16),
            pltpu.VMEM((2, XN, RA, B), BF16),
            pltpu.VMEM((2, 2, R0, B), BF16),
            pltpu.VMEM((2, RA, B), BF16),
            pltpu.VMEM((2, RA, B), BF16),
            pltpu.VMEM((2, 2) + block, BF16),
            pltpu.SemaphoreType.DMA((len(NAMES),)),
            pltpu.SemaphoreType.DMA((len(NAMES),)),
            pltpu.SemaphoreType.DMA((CB + 6 + 2 * OWN,)),
        ],
        compiler_params=pltpu.CompilerParams(
            collective_id=0, has_side_effects=True, vmem_limit_bytes=60 * 1024 * 1024
        ),
    )(place, owner_slot, listing, features, grad_act, weights, factors, roots)
    return pl.pallas_call(
        deliver,
        out_shape=results,
        in_specs=[anywhere] * 2,
        out_specs=(anywhere, anywhere),
        scratch_shapes=[
            pltpu.VMEM((3 * OWN,) + block, BF16),
            pltpu.SemaphoreType.DMA((3 * OWN,)),
            pltpu.SemaphoreType.DMA((3 * OWN,)),
        ],
    )(*made)


def solution(mesh):
    return jax.shard_map(
        body,
        mesh=mesh,
        in_specs=(
            P(None, "rep", None),
            P(None, "rep", "blk"),
            P(None, "blk"),
            P("blk", None),
            P("blk", "rep", None, None, None),
            P("blk", "rep", None, None, None),
            P(),
        ),
        out_specs=(P("blk", "rep", None, None), P("blk", "rep", None, None, None)),
        check_vma=False,
    )
```
